256 devices in a mesh: seq: 16 (over z, core), head: 16 (over x, y).
Axes of the slice: x: 4, y: 4, z: 8, core: 2. Of those that a mesh axis runs over, the one named last changes fastest.
Arguments:
- grad_output: bfloat16 [16384, 4096], P('seq', 'head'), may hold values from -6 to 6
- out_weight: bfloat16 [4096, 8192], P('seq', 'head'), may hold values from -0.0625 to 0.0625
- ssd_out: bfloat16 [16384, 8192], P('seq', 'head'), may hold values from -520 to 520
- gate: bfloat16 [16384, 8192], P('seq', 'head'), may hold values from -5 to 5
- norm_weight: float32 [8192], P('head'), may hold values from 0.5 to 1.5
- time_step: float32 [128, 16384], P('head', 'seq'), may hold values from 0.01 to 0.1
- log_decay: float32 [128, 16384], P('head', 'seq'), may hold values from -0.7 to 0
- state_in: bfloat16 [16384, 8, 128], P('seq'), may hold values from -1.796875 to 1.796875
- state_out: bfloat16 [16384, 8, 128], P('seq'), may hold values from -1.796875 to 1.796875
- skip: float32 [128], P('head'), may hold values from 0.5 to 1.5
Outputs:
- grad_x: bfloat16 [16384, 8192], P('seq', 'head')
- grad_gate: bfloat16 [16384, 8192], P('seq', 'head')
- grad_out_weight: float32 [4096, 8192], P('seq', 'head')
The draws below stay inside these ranges and needn't reach their ends.
All inputs are finite; a program needn't handle non-finite values.
Results may differ from the reference program's by a relative error of at most 0.014.
Values may be sent and summed in bfloat16 or wider, within the bound.
A program may use at most 128 MiB of HBM per device.

```python
import math
from functools import partial
import jax
import jax.numpy as jnp
from jax import lax

D = 4096
HEADS = 128
HDIM = 64
NSTATE = 128
GROUPS = 8
BLOCK_LEN = 256
TOK_DEV = 1024
TOKENS = 16384
DI = 8192


def draw_log_decay(key, part):
    keys = jax.random.split(jax.random.fold_in(key, 11), 7)
    order = jax.random.permutation(keys[0], HEADS)
    slow_count = HEADS // 2
    slow_heads = order < slow_count
    chain = float(TOKENS)
    slow_rate = jnp.exp(jax.random.uniform(keys[1], (HEADS,), jnp.float32, math.log(0.1 / chain), math.log(0.5 / chain)))
    fast_rate = jnp.exp(jax.random.uniform(keys[2], (HEADS,), jnp.float32, math.log(2.0 / chain), math.log(0.035)))
    fading_speed = jnp.where(slow_heads, slow_rate, fast_rate)
    blocks = TOKENS // TOK_DEV
    multiplier_coefficient = jnp.exp2(jax.random.uniform(keys[3], (HEADS, blocks), jnp.float32, -1.0, 1.0))
    multiplier_coefficient = jnp.repeat(multiplier_coefficient, TOK_DEV, axis=1)
    approximate_guess = jax.random.uniform(keys[4], (HEADS, TOKENS), jnp.float32, 0.5, 1.5)
    seat_locations = jax.random.randint(keys[5], (3,), 0, TOKENS)
    increment_lengths = jax.random.uniform(keys[6], (3,), jnp.float32, 0.22, 0.51)
    sequence_indices = jnp.arange(TOKENS)
    clustered_spans = jnp.max(jnp.where(sequence_indices[None, :] == seat_locations[:, None], increment_lengths[:, None], 0.0), axis=0)
    return (-(fading_speed[:, None] * multiplier_coefficient * approximate_guess) - clustered_spans[None, :]).astype(jnp.float32)


def draw_ssd_out(key, part):
    keys = jax.random.split(jax.random.fold_in(key, 23), 4)
    row_scale = jnp.exp(jax.random.uniform(keys[0], (TOKENS,), jnp.float32, 0.0, math.log(10.0)))
    column_scale = jnp.exp(jax.random.uniform(keys[1], (DI,), jnp.float32, math.log(0.3), math.log(3.0)))
    ramp = jnp.arange(DI, dtype=jnp.float32) / DI
    base = jax.random.truncated_normal(keys[3], -4.0, 4.0, (TOKENS, DI), jnp.float32)
    rising = jnp.power(3.0, 0.5 * ramp)
    return (base * row_scale[:, None] * (column_scale * rising)[None, :]).astype(jnp.bfloat16)


def spiked(entries, key, source, target, parts, factor):
    def block_of(dim):
        return (jnp.arange(entries.shape[dim]) // (entries.shape[dim] // parts)).reshape((-1,) + (1,) * (entries.ndim - 1 - dim))

    one_side = jax.random.permutation(key, parts)[block_of(target)]
    other_side = (block_of(target) + parts // 2) % parts
    return jnp.where((block_of(source) == one_side) | (block_of(source) == other_side), factor * entries, entries)


def block_scale(own_key, extent, pieces, low, high):
    def one(dim, blocks):
        steps = jax.random.uniform(jax.random.fold_in(jax.random.fold_in(own_key, 6), dim), (blocks,), jnp.float32, low / len(pieces), high / len(pieces))
        return jnp.repeat(jnp.exp(steps), extent[dim] // blocks).reshape((-1,) + (1,) * (len(extent) - dim - 1))

    level = one(*pieces[0])
    for cut in pieces[1:]:
        level = level * one(*cut)
    return level


def gaussian(own_key, shape, scale, most, shards=(), held_as=jnp.bfloat16):
    loudness = block_scale(own_key, shape, shards, -0.22, 0.18) if shards else 1.0
    drawn = jax.random.normal(own_key, shape, jnp.float32) * scale * loudness
    return jnp.minimum(jnp.maximum(drawn, -most), most).astype(held_as)


def heavy_noise(stream_key, extent, width, bound, cuts, heavy, kind=jnp.bfloat16):
    drawn = width * jax.random.normal(stream_key, extent, jnp.float32)
    if cuts:
        drawn = drawn * block_scale(stream_key, extent, cuts, -0.22, 0.18)
    return jnp.clip(spiked(drawn, jax.random.fold_in(stream_key, 3), *heavy), -bound, bound).astype(kind)


def setup_inputs(seed: int = 0) -> dict:
    seeds = jax.random.split(jax.random.key(seed), 11)
    return {
        "grad_output": heavy_noise(seeds[0], (TOKENS, D), 1.0, 6.0, ((0, 16), (1, 16)), (0, 1, 16, 2.0)),
        "out_weight": gaussian(seeds[1], (D, DI), DI ** -0.5, 0.0625, ((0, 16), (1, 16))),
        "ssd_out": draw_ssd_out(jax.random.fold_in(seeds[10], 71), 0),
        "gate": gaussian(seeds[3], (TOKENS, DI), 1.0, 5.0, ((0, 16), (1, 16))),
        "norm_weight": jnp.clip(1.0 + 0.1 * jax.random.normal(seeds[4], (DI,), jnp.float32), 0.5, 1.5),
        "time_step": jnp.clip(jnp.exp(math.log(0.1) - 2.3025851 * jax.random.uniform(seeds[5], (HEADS, TOKENS), jnp.float32) ** block_scale(seeds[5], (HEADS, TOKENS), ((0, 16), (1, 16)), -0.2, 0.2)), 0.01, 0.1),
        "log_decay": draw_log_decay(jax.random.fold_in(seeds[10], 71), 0),
        "state_in": gaussian(seeds[7], (TOKENS, GROUPS, NSTATE), 0.3, 1.796875, ((0, 16),)),
        "state_out": gaussian(seeds[8], (TOKENS, GROUPS, NSTATE), 0.3, 1.796875, ((0, 16),)),
        "skip": jnp.clip(0.5 + 1.0 * jax.random.uniform(seeds[9], (HEADS,), jnp.float32) ** block_scale(seeds[9], (HEADS,), ((0, 16),), -0.2, 0.2), 0.5, 1.5),
    }


epsilon = 1e-05

def head_grad(head, grad_ssd, time_step, log_decay, state_in, state_out, skip):
    group = (head // (HEADS // GROUPS)).astype(jnp.int32)
    blocks = TOKENS // BLOCK_LEN
    start_col = (head * HDIM).astype(jnp.int32)
    grad_cols = lax.dynamic_slice_in_dim(grad_ssd, start_col, HDIM, 1).astype(jnp.float32)
    grad_cols = grad_cols.reshape(blocks, BLOCK_LEN, HDIM)
    b_rows = lax.dynamic_index_in_dim(state_in, group, 1, keepdims=False).astype(jnp.float32)
    b_rows = b_rows.reshape(blocks, BLOCK_LEN, NSTATE)
    c_rows = lax.dynamic_index_in_dim(state_out, group, 1, keepdims=False).astype(jnp.float32)
    c_rows = c_rows.reshape(blocks, BLOCK_LEN, NSTATE)
    rates = lax.dynamic_index_in_dim(log_decay, head, 0, keepdims=False).reshape(blocks, BLOCK_LEN)
    step_sizes = lax.dynamic_index_in_dim(time_step, head, 0, keepdims=False).reshape(blocks, BLOCK_LEN)
    skip_head = lax.dynamic_index_in_dim(skip, head, 0, keepdims=False)
    cumulative = jnp.cumsum(rates, axis=1)
    block_total = cumulative[:, -1]
    sequence_indices = jnp.arange(BLOCK_LEN)
    upper_mask = sequence_indices[None, :] >= sequence_indices[:, None]
    scores = jnp.einsum('ktn,ksn->kts', b_rows, c_rows)
    log_gap = cumulative[:, None, :] - cumulative[:, :, None]
    block_weights = jnp.where(upper_mask, scores * jnp.exp(jnp.minimum(log_gap, 0.0)), 0.0).astype(jnp.bfloat16)
    block_weights = lax.optimization_barrier(block_weights).astype(jnp.float32)
    within = jnp.einsum('kts,ksp->ktp', block_weights, grad_cols)
    scaled = (jnp.exp(cumulative)[:, :, None] * grad_cols).astype(jnp.bfloat16)
    scaled = lax.optimization_barrier(scaled).astype(jnp.float32)
    block_state = jnp.einsum('ksp,ksn->kpn', scaled, c_rows)

    def fold_block(carried, inputs):
        state_now, total_now = inputs
        return (state_now + jnp.exp(total_now) * carried, carried)
    unused, carry = lax.scan(fold_block, jnp.zeros((HDIM, NSTATE), jnp.float32), (block_state, block_total), reverse=True)
    carry_low = lax.optimization_barrier(carry.astype(jnp.bfloat16)).astype(jnp.float32)
    across = jnp.einsum('kpn,ktn->ktp', carry_low, b_rows) * jnp.exp(block_total[:, None] - cumulative)[:, :, None]
    result = step_sizes[:, :, None] * (within + across) + skip_head * grad_cols
    return result.reshape(TOKENS, HDIM).astype(jnp.bfloat16)

def reference(grad_output, out_weight, ssd_out, gate, norm_weight, time_step, log_decay, state_in, state_out, skip):
    values = ssd_out.astype(jnp.float32)
    gate_values = gate.astype(jnp.float32)
    sigmoid_gate = jax.nn.sigmoid(gate_values)
    silu_gate = gate_values * sigmoid_gate
    gated_values = values * silu_gate
    inverse_rms = lax.rsqrt(lax.optimization_barrier(jnp.mean(gated_values * gated_values, axis=1, keepdims=True)) + epsilon)
    normed = (gated_values * inverse_rms * norm_weight).astype(jnp.bfloat16)
    normed_grad = jnp.dot(grad_output, out_weight, preferred_element_type=jnp.float32)
    weighted = lax.optimization_barrier(jnp.sum(norm_weight * normed_grad * gated_values, axis=1, keepdims=True))
    gated_grad = inverse_rms * norm_weight * normed_grad - gated_values * inverse_rms ** 3 * weighted / DI
    grad_gate = (gated_grad * values * sigmoid_gate * (1.0 + gate_values * (1.0 - sigmoid_gate))).astype(jnp.bfloat16)
    grad_ssd = (gated_grad * silu_gate).astype(jnp.bfloat16)
    grad_out_weight = jnp.dot(grad_output.T, normed, preferred_element_type=jnp.float32) * (1.0 / math.sqrt(TOKENS))
    per_head = lax.map(partial(head_grad, grad_ssd=grad_ssd, time_step=time_step, log_decay=log_decay, state_in=state_in, state_out=state_out, skip=skip), jnp.arange(HEADS, dtype=jnp.int32))
    grad_x = jnp.transpose(per_head, (1, 0, 2)).reshape(TOKENS, DI)
    return (grad_x, grad_gate, grad_out_weight)
```

```python
import functools
import math

import jax
import jax.numpy as jnp
from jax import lax
from jax.experimental import pallas as pl
from jax.experimental.pallas import tpu as pltpu
from jax.sharding import Mesh
from jax.sharding import PartitionSpec as P

EPS = 1e-05
F32, BF16 = jnp.float32, jnp.bfloat16
MESH = pl.DeviceIdType.MESH
BLK = 256
A, B = (0, 512), (512, 512)
A0, A1, B0, B1 = (0, 256), (256, 256), (512, 256), (768, 256)
STEP = ((1, 0), (-1, 0), (0, 1), (0, -1))
ITEMS = (
    ((0, 0, A), (0, 0, B), (-1, 0, A), (0, 1, B), (0, -1, B), (0, 2, B), (-1, 1, B0), (-1, -1, B0), (-1, 2, B0)),
    ((0, 0, A), (0, 0, B), (1, 0, B), (0, 1, B), (0, -1, B), (0, 2, B), (1, 1, B1), (1, -1, B1), (1, 2, B1)),
    ((0, 0, B), (0, 0, A), (0, -1, A), (1, 0, A), (-1, 0, A), (2, 0, A), (1, -1, A0), (-1, -1, A0), (2, -1, A0)),
    ((0, 0, B), (0, 0, A), (0, 1, B), (1, 0, A), (-1, 0, A), (2, 0, A), (1, 1, A1), (-1, 1, A1), (2, 1, A1)),
)
PAIRS = (
    ((0, 0), (0, 1)),
    ((1, 0), (0, -1)),
    ((-1, 0), (1, 1)),
    ((2, 0), (-1, 1)),
    ((0, 2), (1, -1)),
    ((1, 2), (-1, -1)),
    ((-1, 2), (2, 1)),
    ((2, 2), (2, -1)),
)
ECUM, ETAIL, TSTEP, CUM = 0, 24, 48, 72


def split3(q):
    first = q.astype(BF16).astype(F32)
    second = (q - first).astype(BF16).astype(F32)
    third = (q - first - second).astype(BF16).astype(F32)
    return [first, second, third]


def fold_lanes(v):
    return (v[:, 0:128] + v[:, 128:256]) + (v[:, 256:384] + v[:, 384:512])


def kernel(
    a_hbm, w_hbm, so_hbm, gt_hbm, nw_ref, ts_ref, ld_ref, bin_hbm, cin_hbm, skip_ref,
    gx_hbm, gg_hbm, gw_hbm,
    abuf, wbuf, so, gt, gated, silu, fgate, ng, ecw, etw, tsw, wts, gkeep, gout, gin, fromr, froml,
    normt, stage, conv, bsel, csel, ct, qt, cum_s, col, sqs, wds, st, schip, s0buf, d0buf, carry, msend, csend, gw,
    a_ssem, a_rsem, w_ssem, w_rsem, b_ssem, b_rsem, r_ssem, r_rsem, g_ssem, g_rsem, h_ssem, h_rsem,
    d_ssem, d_rsem, s_ssem, s_rsem, c_ssem, c_rsem, m_ssem, l_sem,
):
    z, c, x, y = (lax.axis_index(n) for n in ("z", "c", "x", "y"))
    head = x * 4 + y

    def at(dz=0, dc=0, dx=0, dy=0):
        return ((z + dz + 8) % 8, (c + dc) % 2, (x + dx + 4) % 4, (y + dy + 4) % 4)

    def slot(dx, dy):
        return ((x + dx + 4) % 4) * 4 + (y + dy + 4) % 4

    def remote(src, dst, ssem, rsem, dev):
        return pltpu.make_async_remote_copy(
            src_ref=src, dst_ref=dst, send_sem=ssem, recv_sem=rsem, device_id=dev, device_id_type=MESH
        )

    loads = [
        pltpu.make_async_copy(a_hbm, abuf.at[head], l_sem.at[0]),
        pltpu.make_async_copy(w_hbm, wbuf.at[z * 2 + c], l_sem.at[1]),
        pltpu.make_async_copy(so_hbm, so, l_sem.at[2]),
        pltpu.make_async_copy(gt_hbm, gt, l_sem.at[3]),
        pltpu.make_async_copy(bin_hbm, stage.at[0], l_sem.at[4]),
        pltpu.make_async_copy(cin_hbm, stage.at[1], l_sem.at[5]),
    ]
    for load in loads:
        load.start()
    barrier = pltpu.get_barrier_semaphore()

    def greet(k, carry_):
        other = (head + k) % 16
        pl.semaphore_signal(barrier, inc=1, device_id=(z, c, other // 4, other % 4), device_id_type=MESH)
        return carry_

    lax.fori_loop(1, 16, greet, 0)
    for dev in (at(dz=1), at(dz=-1), at(dc=1)):
        pl.semaphore_signal(barrier, inc=1, device_id=dev, device_id_type=MESH)
    loads[0].wait()
    loads[1].wait()
    pl.semaphore_wait(barrier, 18)

    def a_copy(d, k, got):
        dx, dy, (row, n) = ITEMS[d][k]
        sx, sy = STEP[d]
        here = slot(dx - sx, dy - sy) if got else slot(dx, dy)
        piece = abuf.at[here, pl.ds(row, n)]
        return remote(piece, piece, a_ssem.at[d, k], a_rsem.at[d, k], at(dx=sx, dy=sy))

    def a_send(*flows):
        for d, k in flows:
            a_copy(d, k, False).start()

    def a_wait(*flows):
        for d, k in flows:
            a_copy(d, k, True).wait_recv()

    every = lambda k: [(d, k) for d in range(4)]

    def w_copy(d, k, got):
        sign = 1 if d == 0 else -1
        far = (k // 2 if k < 6 else 3) + (1 if got else 0)
        half = k % 2 if k < 6 else d
        here = ((z - sign * far + 8) % 8) * 2 + c
        piece = wbuf.at[here, pl.ds(half * 128, 128)]
        return remote(piece, piece, w_ssem.at[d, k], w_rsem.at[d, k], at(dz=sign))

    def b_copy(k, got):
        here = ((z + k) % 8) * 2 + ((c + 1) % 2 if got else c)
        return remote(wbuf.at[here], wbuf.at[here], b_ssem.at[k], b_rsem.at[k], at(dc=1))

    def w_event(k):
        for d in (0, 1):
            w_copy(d, k, True).wait_recv()
            if k < 4:
                w_copy(d, k + 2, False).start()
        if k == 4:
            w_copy(0, 6, False).start()
        if k == 5:
            w_copy(1, 6, False).start()
        if k in (1, 3, 5):
            b_copy((k + 1) // 2, False).start()
            b_copy(8 - (k + 1) // 2, False).start()
        if k == 6:
            b_copy(4, False).start()

    a_send(*every(0), *every(1))
    for k in (0, 1):
        for d in (0, 1):
            w_copy(d, k, False).start()
    b_copy(0, False).start()

    def row_copy(slots, ssem, rsem, k, got):
        other = (head + k) % 16
        source = (head + 16 - k) % 16
        here = source if got else head
        return remote(slots.at[here], slots.at[here], ssem.at[k], rsem.at[k], (z, c, other // 4, other % 4))

    def row_send(slots, ssem, rsem):
        def one(k, carry_):
            row_copy(slots, ssem, rsem, k, False).start()
            return carry_

        lax.fori_loop(1, 16, one, 0)

    def row_sum(slots, ssem, rsem):
        def one(k, carry_):
            copy = row_copy(slots, ssem, rsem, k, True)
            copy.wait_recv()
            return carry_

        lax.fori_loop(1, 16, one, 0)
        total = slots[0]
        for k in range(1, 16):
            total = total + slots[k]
        return total

    def row_done(slots, ssem, rsem):
        def one(k, carry_):
            row_copy(slots, ssem, rsem, k, False).wait_send()
            return carry_

        lax.fori_loop(1, 16, one, 0)

    def to_column(row):
        return jnp.broadcast_to(row, (128, row.shape[1])).T

    def rows128(r):
        return pl.ds(pl.multiple_of(r * 128, 128), 128)

    loads[2].wait()
    loads[3].wait()

    @pl.loop(0, 8)
    def _(r):
        rows = rows128(r)
        values = so[rows, :].astype(F32)
        gate_values = gt[rows, :].astype(F32)
        sig = jax.nn.sigmoid(gate_values)
        sl = gate_values * sig
        gv = values * sl
        gated[rows, :] = gv
        silu[rows, :] = sl
        fgate[rows, :] = values * sig * (1.0 + gate_values * (1.0 - sig))
        sqs[head, :, rows] = jnp.sum(fold_lanes(gv * gv).T, axis=0, keepdims=True)

    row_send(sqs, g_ssem, g_rsem)
    w_event(0)

    rows_i = lax.broadcasted_iota(jnp.int32, (BLK, BLK), 0)
    cols_i = lax.broadcasted_iota(jnp.int32, (BLK, BLK), 1)
    tri = (rows_i <= cols_i).astype(F32).astype(BF16)
    for k in range(4):
        cols = slice(k * BLK, (k + 1) * BLK)
        parts = jnp.concatenate(split3(ld_ref[:, cols]), axis=0).astype(BF16)
        summed = jnp.dot(parts, tri, preferred_element_type=F32)
        cum = summed[0:8] + summed[8:16] + summed[16:24]
        cum_s[:, cols] = cum
        total = cum[:, BLK - 1 : BLK]
        table = (
            split3(jnp.exp(cum))
            + split3(jnp.exp(total - cum))
            + split3(ts_ref[:, cols])
            + [cum, jnp.zeros((128 - CUM - 8, BLK), F32)]
        )
        qt[cols, :] = jnp.concatenate(table, axis=0).T
    lane_head = lax.broadcasted_iota(jnp.int32, (128, 512), 1) // 64
    part_row = lax.broadcasted_iota(jnp.int32, (128, 512), 0)

    def pick(first):
        inside = (part_row >= first) & (part_row < first + 24) & ((part_row - first) % 8 == lane_head)
        return inside.astype(F32).astype(BF16)

    for first, wide in ((ECUM, ecw), (ETAIL, etw), (TSTEP, tsw)):
        chosen = pick(first)

        @pl.loop(0, 4)
        def _(k, chosen=chosen, wide=wide):
            rows = pl.ds(pl.multiple_of(k * BLK, BLK), BLK)
            wide[rows, :] = jnp.dot(qt[rows, :].astype(BF16), chosen, preferred_element_type=F32)

    decay_all = ecw[255:256, :] * ecw[511:512, :] * ecw[767:768, :] * ecw[1023:1024, :]
    d0buf[0] = decay_all

    a_wait(*every(0))
    a_send((0, 2), (0, 3), (0, 4), (1, 3), (3, 2), (3, 3), (3, 4), (2, 3))
    w_event(1)

    group = head // 2
    for which, (load, sel) in enumerate(((loads[4], bsel), (loads[5], csel))):
        load.wait()

        @pl.loop(0, 4)
        def _(r, which=which, sel=sel):
            conv[...] = stage[which, pl.ds(pl.multiple_of(r * 2048, 2048), 2048), :].astype(F32)
            sel[pl.ds(pl.multiple_of(r * 256, 256), 256), :] = conv[pl.ds(group, 256, stride=8), :].astype(BF16)

    mean = row_sum(sqs, g_ssem, g_rsem) * (1.0 / 8192)
    col[...] = to_column(lax.rsqrt(mean + EPS))
    w_event(2)
    nw = nw_ref[...]

    @pl.loop(0, 8)
    def _(r):
        rows = rows128(r)
        inv = col[rows, :][:, 0:1]
        normed = gated[rows, :] * inv * nw
        normt[:, rows] = normed.T.astype(BF16)

    ct[...] = csel[...].astype(F32).T.astype(BF16)

    a_wait(*every(1))
    a_send((1, 2), (1, 4), (2, 2), (2, 4))
    w_event(3)

    def pair_slots(p):
        (ex, ey), (ox, oy) = PAIRS[p]
        return slot(ex, ey), slot(ox, oy)

    def give_copy(p):
        return remote(gout.at[p], gin.at[p], h_ssem.at[p], h_rsem.at[p], at(dc=1))

    def weight_part(p):
        first, second = pair_slots(p)
        swap = (y + PAIRS[p][0][1] + 4 + c) % 2
        mine = jnp.where(swap == 0, first, second)
        other = jnp.where(swap == 0, second, first)

        @pl.loop(0, 4)
        def _(r):
            rows = rows128(r)
            lhs = normt[rows, :]
            gout[p, rows, :] = jnp.dot(lhs, abuf[other], preferred_element_type=F32).astype(BF16)
            gkeep[p, rows, :] = jnp.dot(lhs, abuf[mine], preferred_element_type=F32).astype(BF16)

        give_copy(p).start()

    def grad_part(p):
        first, second = pair_slots(p)

        @pl.loop(0, 4)
        def _(r):
            rows = pl.ds(pl.multiple_of(r * 256, 256), 256)
            add = jnp.dot(abuf[first, rows, :], wbuf[first], preferred_element_type=F32)
            add = add + jnp.dot(abuf[second, rows, :], wbuf[second], preferred_element_type=F32)
            if p == 0:
                ng[rows, :] = add
            else:
                ng[rows, :] += add

    def root_of(p):
        first, second = pair_slots(p)
        swap = (y + PAIRS[p][0][1] + 4 + c) % 2
        return jnp.where(swap == 0, first, second) // 2

    roots = [root_of(p) for p in range(8)]

    def tab(p):
        found = roots[0]
        for q in range(1, 8):
            found = jnp.where(p == q, roots[q], found)
        return found

    def r_copy(p, i, rightward, right_buf):
        piece = pl.ds(i * 256, 256)
        dev = ((z + jnp.where(rightward, 1, 7)) % 8, c, x, y)
        buf = fromr if right_buf else froml
        return remote(
            gkeep.at[p, piece], buf.at[p, piece], r_ssem.at[p, i], r_rsem.at[p, i, 0 if right_buf else 1], dev
        )

    def combine(p):
        give_copy(p).wait_recv()
        gkeep[p] = (gkeep[p].astype(F32) + gin[p].astype(F32)).astype(BF16)

    def rs_level(p, lev):
        rel = (z - tab(p) + 8) % 8
        for i in (0, 1):
            piece = pl.ds(i * 256, 256)
            rightward = rel >= 4 + i
            level = jnp.where(rightward, rel - (4 + i), (3 + i) - rel)

            def hop(right_buf, p=p, i=i, piece=piece):
                copy = r_copy(p, i, right_buf, right_buf)

                @pl.when(lev > 0)
                def _():
                    copy.wait_recv()
                    buf = fromr if right_buf else froml
                    gkeep[p, piece, :] = (gkeep[p, piece, :].astype(F32) + buf[p, piece, :].astype(F32)).astype(BF16)

                copy.start()

            live = (rel != 0) & (level == lev)

            @pl.when(live & rightward)
            def _():
                hop(True)

            @pl.when(live & jnp.logical_not(rightward))
            def _():
                hop(False)

        @pl.when((rel == 0) & (lev == 4))
        def _():
            for i in (0, 1):
                piece = pl.ds(i * 256, 256)
                r_copy(p, i, True, True).wait_recv()
                r_copy(p, i, False, False).wait_recv()
                gw[piece, :] = (
                    gkeep[p, piece, :].astype(F32) + fromr[p, piece, :].astype(F32) + froml[p, piece, :].astype(F32)
                ) * (1.0 / math.sqrt(16384.0))

    def rs_stage(t):
        if 0 < t <= 8:
            combine(t - 1)

        def one(lev, carry_):
            p = t - 1 - lev

            @pl.when((p >= 0) & (p < 8))
            def _():
                rs_level(p, lev)

            return carry_

        lax.fori_loop(0, 5, one, 0)

    def r_done():
        def one(p, carry_):
            rel = (z - tab(p) + 8) % 8

            @pl.when(rel != 0)
            def _():
                for i in (0, 1):
                    r_copy(p, i, True, True).wait_send()

            give_copy(p).wait_send()
            return carry_

        lax.fori_loop(0, 8, one, 0)

    weight_part(0)
    w_event(4)
    weight_part(1)
    a_wait((0, 2), (3, 2), (1, 3), (2, 3))
    a_send(*every(5))
    w_event(5)
    rs_stage(1)

    keep_upper = cols_i >= rows_i

    @pl.loop(0, 4)
    def _(k):
        rows = pl.ds(pl.multiple_of(k * BLK, BLK), BLK)
        scores = lax.dot_general(bsel[rows, :], csel[rows, :], (((1,), (1,)), ((), ())), preferred_element_type=F32)
        columns = qt[rows, :]
        for h in range(8):
            gap = cum_s[h : h + 1, rows] - columns[:, CUM + h : CUM + h + 1]
            weight = jnp.where(keep_upper, scores * jnp.exp(jnp.minimum(gap, 0.0)), 0.0)
            wts[k, h] = weight.astype(BF16)

    w_event(6)
    a_wait((0, 3), (1, 2), (2, 2), (3, 3))
    a_send(*every(6))
    weight_part(2)
    rs_stage(2)
    for k in range(8):
        b_copy(k, True).wait_recv()
    grad_part(0)
    grad_part(1)
    grad_part(2)
    a_wait(*every(4))
    a_send(*every(7))
    weight_part(3)
    rs_stage(3)
    grad_part(3)
    weight_part(4)
    rs_stage(4)
    a_wait(*every(5))
    a_send(*every(8))
    grad_part(4)
    a_wait(*every(6))
    weight_part(5)
    grad_part(5)
    a_wait(*every(7))
    weight_part(6)
    rs_stage(5)
    grad_part(6)
    a_wait(*every(8))
    grad_part(7)

    @pl.loop(0, 8)
    def _(r):
        rows = rows128(r)
        term = nw_ref[...] * ng[rows, :] * gated[rows, :]
        wds[head, :, rows] = jnp.sum(fold_lanes(term).T, axis=0, keepdims=True)

    row_send(wds, d_ssem, d_rsem)
    weight_part(7)
    rs_stage(6)
    weighted = row_sum(wds, d_ssem, d_rsem)

    cube = to_column(weighted * (1.0 / 8192))

    gs = gt

    for r in range(8):
        rows = slice(r * 128, (r + 1) * 128)
        inv = col[rows, 0:1]
        wcol = cube[rows, 0:1]
        gg = inv * nw_ref[...] * ng[rows, :] - gated[rows, :] * (inv * inv * inv * wcol)
        so[rows, :] = (gg * fgate[rows, :]).astype(BF16)
        gs[rows, :] = (gg * silu[rows, :]).astype(BF16)
    gate_out = pltpu.make_async_copy(so, gg_hbm, l_sem.at[0])
    gate_out.start()

    @pl.loop(0, 4)
    def _(k):
        rows = pl.ds(pl.multiple_of(k * BLK, BLK), BLK)
        scaled = (ecw[rows, :] * gs[rows, :].astype(F32)).astype(BF16)
        st[k] = jnp.dot(ct[:, rows], scaled, preferred_element_type=F32)

    ends = [ecw[k * BLK + BLK - 1 : k * BLK + BLK, :] for k in range(4)]

    def summary():
        return st[0] + ends[0] * (st[1] + ends[1] * (st[2] + ends[2] * st[3]))

    def s0_copy():
        return remote(msend, s0buf, s_ssem.at[0], s_rsem.at[0], (z, 1, x, y))

    def d0_copy():
        return remote(d0buf.at[0], d0buf.at[1], s_ssem.at[1], s_rsem.at[1], (z, 1, x, y))

    def chain_copy(q):
        piece = pl.ds(q * 32, 32)
        return remote(msend.at[piece], carry.at[piece], m_ssem.at[q], c_rsem.at[q], ((z + 7) % 8, 1, x, y))

    def core_copy(q):
        piece = pl.ds(q * 32, 32)
        return remote(csend.at[piece], carry.at[piece], c_ssem.at[q], c_rsem.at[q], (z, 0, x, y))

    @pl.when(c == 0)
    def _():
        msend[...] = summary().astype(BF16)
        d0_copy().start()
        s0_copy().start()

    @pl.when(c == 1)
    def _():
        schip[...] = summary()

    def within_all():
        low = lax.broadcasted_iota(jnp.int32, (BLK, 128), 1) < 64

        @pl.loop(0, 4)
        def _(k):
            rows = pl.ds(pl.multiple_of(k * BLK, BLK), BLK)
            for hp in range(4):
                cols = slice(hp * 128, hp * 128 + 128)
                g = gs[rows, cols]
                zero = jnp.zeros_like(g)
                ng[rows, cols] = jnp.dot(
                    wts[k, 2 * hp], jnp.where(low, g, zero), preferred_element_type=F32
                ) + jnp.dot(wts[k, 2 * hp + 1], jnp.where(low, zero, g), preferred_element_type=F32)

    def drain():
        for t in range(7, 13):
            rs_stage(t)

    ahead = (z >= 6) & (c == 1)

    @pl.when(jnp.logical_not(ahead))
    def _():
        within_all()

    @pl.when(c == 1)
    def _():
        d0_copy().wait_recv()
        s0_copy().wait_recv()
        d0 = d0buf[1]
        d1 = d0buf[0]
        for q in range(4):
            piece = pl.ds(q * 32, 32)

            @pl.when(z < 7)
            def _():
                chain_copy(q).wait_recv()

            @pl.when(z == 7)
            def _():
                carry[piece, :] = jnp.zeros((32, 512), BF16)

            own = schip[piece, :]
            after = own + d1 * carry[piece, :].astype(F32)
            msend[piece, :] = (s0buf[piece, :].astype(F32) + d0 * after).astype(BF16)
            csend[piece, :] = after.astype(BF16)

            @pl.when(z > 0)
            def _():
                chain_copy(q).start()

            core_copy(q).start()

    @pl.when(ahead)
    def _():
        within_all()

    drain()
    gw_out = pltpu.make_async_copy(gw, gw_hbm, l_sem.at[1])
    gw_out.start()

    @pl.when(c == 0)
    def _():
        for q in range(4):
            core_copy(q).wait_recv()

    lane512 = lax.broadcasted_iota(jnp.int32, (1, 512), 1) // 64
    skw = jnp.zeros((1, 512), F32)
    for h in range(8):
        skw = jnp.where(lane512 == h, skip_ref[0, h], skw)
    state = carry[...].astype(F32)
    for k in (3, 2, 1, 0):
        rows = slice(k * BLK, (k + 1) * BLK)
        across = jnp.dot(bsel[rows, :], state.astype(BF16), preferred_element_type=F32)
        if k:
            state = st[k] + ends[k] * state
        out = tsw[rows, :] * (ng[rows, :] + etw[rows, :] * across) + skw * gs[rows, :].astype(F32)
        so_rows = out.astype(BF16)
        if k == 3:
            gate_out.wait()
        so[rows, :] = so_rows
    x_out = pltpu.make_async_copy(so, gx_hbm, l_sem.at[2])
    x_out.start()

    for d in range(4):
        for k in range(9):
            a_copy(d, k, False).wait_send()
    for d in (0, 1):
        for k in range(7):
            w_copy(d, k, False).wait_send()
    for k in range(8):
        b_copy(k, False).wait_send()
    row_done(sqs, g_ssem, g_rsem)
    row_done(wds, d_ssem, d_rsem)
    r_done()

    @pl.when(c == 0)
    def _():
        d0_copy().wait_send()
        s0_copy().wait_send()

    @pl.when(c == 1)
    def _():
        for q in range(4):
            core_copy(q).wait_send()

            @pl.when(z > 0)
            def _():
                chain_copy(q).wait_send()

    gw_out.wait()
    x_out.wait()


def on_device(a, w, so, gt, nw, ts, ld, bin_, cin, skip):
    any_ = pl.BlockSpec(memory_space=pl.ANY)
    vmem = pl.BlockSpec(memory_space=pltpu.VMEM)
    smem = pl.BlockSpec(memory_space=pltpu.SMEM)
    V, D = pltpu.VMEM, pltpu.SemaphoreType.DMA
    gx, gg, gwt = pl.pallas_call(
        kernel,
        out_shape=(
            jax.ShapeDtypeStruct((1024, 512), BF16),
            jax.ShapeDtypeStruct((1024, 512), BF16),
            jax.ShapeDtypeStruct((512, 256), F32),
        ),
        in_specs=[any_, any_, any_, any_, vmem, vmem, vmem, any_, any_, smem],
        out_specs=(any_, any_, any_),
        scratch_shapes=[
            V((16, 1024, 256), BF16), V((16, 256, 512), BF16), V((1024, 512), BF16), V((1024, 512), BF16),
            V((1024, 512), F32), V((1024, 512), F32), V((1024, 512), F32), V((1024, 512), F32),
            V((1024, 512), F32), V((1024, 512), F32), V((1024, 512), F32), V((4, 8, 256, 256), BF16),
            V((8, 512, 256), BF16), V((8, 512, 256), BF16), V((8, 512, 256), BF16), V((8, 512, 256), BF16),
            V((8, 512, 256), BF16),
            V((512, 1024), BF16), V((2, 8192, 128), BF16), V((2048, 128), F32), V((1024, 128), BF16),
            V((1024, 128), BF16), V((128, 1024), BF16), V((1024, 128), F32), V((8, 1024), F32), V((1024, 128), F32),
            V((16, 1, 1024), F32), V((16, 1, 1024), F32), V((4, 128, 512), F32), V((128, 512), F32),
            V((128, 512), BF16), V((2, 1, 512), F32), V((128, 512), BF16), V((128, 512), BF16), V((128, 512), BF16),
            V((512, 256), F32),
            D((4, 9)), D((4, 9)), D((2, 7)), D((2, 7)), D((8,)), D((8,)), D((8, 2)), D((8, 2, 2)), D((16,)), D((16,)),
            D((8,)), D((8,)), D((16,)), D((16,)), D((2,)), D((2,)), D((4,)), D((4,)), D((4,)), D((6,)),
        ],
        compiler_params=pltpu.CompilerParams(
            collective_id=0, has_side_effects=True, vmem_limit_bytes=67043328
        ),
        name="mixer_backward",
    )(
        a, w, so, gt, nw.reshape(1, 512), ts, ld, bin_.reshape(8192, 128), cin.reshape(8192, 128), skip.reshape(1, 8)
    )
    return gx, gg, gwt.T


def solution(mesh):
    finer = Mesh(mesh.devices.reshape(8, 2, 4, 4), ("z", "c", "x", "y"))
    seq, heads = ("z", "c"), ("x", "y")
    return jax.shard_map(
        on_device,
        mesh=finer,
        in_specs=(
            P(seq, heads), P(seq, heads), P(seq, heads), P(seq, heads), P(heads), P(heads, seq), P(heads, seq),
            P(seq, None, None), P(seq, None, None), P(heads),
        ),
        out_specs=(P(seq, heads), P(seq, heads), P(seq, heads)),
        check_vma=False,
    )
```

```python
import functools
import math

import jax
import jax.numpy as jnp
from jax import lax
from jax.experimental import pallas as pl
from jax.experimental.pallas import tpu as pltpu
from jax.sharding import Mesh
from jax.sharding import PartitionSpec as P

EPS = 1e-05
F32, BF16 = jnp.float32, jnp.bfloat16
MESH = pl.DeviceIdType.MESH
BLK = 256
A, B = (0, 512), (512, 512)
A0, A1, B0, B1 = (0, 256), (256, 256), (512, 256), (768, 256)
STEP = ((1, 0), (-1, 0), (0, 1), (0, -1))
ITEMS = (
    ((0, 0, A), (0, 0, B), (-1, 0, A), (0, 1, B), (0, -1, B), (0, 2, B), (-1, 1, B0), (-1, -1, B0), (-1, 2, B0)),
    ((0, 0, A), (0, 0, B), (1, 0, B), (0, 1, B), (0, -1, B), (0, 2, B), (1, 1, B1), (1, -1, B1), (1, 2, B1)),
    ((0, 0, B), (0, 0, A), (0, -1, A), (1, 0, A), (-1, 0, A), (2, 0, A), (1, -1, A0), (-1, -1, A0), (2, -1, A0)),
    ((0, 0, B), (0, 0, A), (0, 1, B), (1, 0, A), (-1, 0, A), (2, 0, A), (1, 1, A1), (-1, 1, A1), (2, 1, A1)),
)
PAIRS = (
    ((0, 0), (0, 1)),
    ((1, 0), (0, -1)),
    ((-1, 0), (1, 1)),
    ((2, 0), (-1, 1)),
    ((0, 2), (1, -1)),
    ((1, 2), (-1, -1)),
    ((-1, 2), (2, 1)),
    ((2, 2), (2, -1)),
)
ECUM, ETAIL, TSTEP, CUM = 0, 24, 48, 72


def split3(q):
    first = q.astype(BF16).astype(F32)
    second = (q - first).astype(BF16).astype(F32)
    third = (q - first - second).astype(BF16).astype(F32)
    return [first, second, third]


def scoped(fn):
    @functools.wraps(fn)
    def wrapped(*args):
        with jax.named_scope(fn.__name__):
            return fn(*args)

    return wrapped


def fold_lanes(v):
    return (v[:, 0:128] + v[:, 128:256]) + (v[:, 256:384] + v[:, 384:512])


def kernel(
    a_hbm, w_hbm, so_hbm, gt_hbm, nw_ref, ts_ref, ld_ref, bin_hbm, cin_hbm, skip_ref,
    gx_hbm, gg_hbm, gw_hbm,
    abuf, wbuf, so, gt, gated, silu, fgate, ng, ecw, etw, tsw, wts, gkeep, gout, gin, fromz,
    normt, stage, conv, bsel, csel, ct, qt, cum_s, col, sqs, wds, st, acc, s0buf, d0buf, sall, dall, weight, carry, gw,
    a_ssem, a_rsem, w_ssem, w_rsem, b_ssem, b_rsem, r_ssem, r_rsem, g_ssem, g_rsem, h_ssem, h_rsem,
    d_ssem, d_rsem, s_ssem, s_rsem, c_ssem, c_rsem, m_ssem, m_rsem, e_ssem, e_rsem, l_sem,
):
    z, c, x, y = (lax.axis_index(n) for n in ("z", "c", "x", "y"))
    head = x * 4 + y

    def at(dz=0, dc=0, dx=0, dy=0):
        return ((z + dz + 8) % 8, (c + dc) % 2, (x + dx + 4) % 4, (y + dy + 4) % 4)

    def slot(dx, dy):
        return ((x + dx + 4) % 4) * 4 + (y + dy + 4) % 4

    def remote(src, dst, ssem, rsem, dev):
        return pltpu.make_async_remote_copy(
            src_ref=src, dst_ref=dst, send_sem=ssem, recv_sem=rsem, device_id=dev, device_id_type=MESH
        )

    loads = [
        pltpu.make_async_copy(a_hbm, abuf.at[head], l_sem.at[0]),
        pltpu.make_async_copy(w_hbm, wbuf.at[z * 2 + c], l_sem.at[1]),
        pltpu.make_async_copy(so_hbm, so, l_sem.at[2]),
        pltpu.make_async_copy(gt_hbm, gt, l_sem.at[3]),
        pltpu.make_async_copy(bin_hbm, stage.at[0], l_sem.at[4]),
        pltpu.make_async_copy(cin_hbm, stage.at[1], l_sem.at[5]),
    ]
    for load in loads:
        load.start()
    barrier = pltpu.get_barrier_semaphore()

    def greet(k, carry_):
        other = (head + k) % 16
        pl.semaphore_signal(barrier, inc=1, device_id=(z, c, other // 4, other % 4), device_id_type=MESH)
        return carry_

    lax.fori_loop(1, 16, greet, 0)
    for dev in (at(dz=1), at(dz=-1), at(dc=1)):
        pl.semaphore_signal(barrier, inc=1, device_id=dev, device_id_type=MESH)
    with jax.named_scope("entry"):
        loads[0].wait()
        loads[1].wait()
        pl.semaphore_wait(barrier, 18)

    def a_copy(d, k, got):
        dx, dy, (row, n) = ITEMS[d][k]
        sx, sy = STEP[d]
        here = slot(dx - sx, dy - sy) if got else slot(dx, dy)
        piece = abuf.at[here, pl.ds(row, n)]
        return remote(piece, piece, a_ssem.at[d, k], a_rsem.at[d, k], at(dx=sx, dy=sy))

    def a_send(*flows):
        for d, k in flows:
            a_copy(d, k, False).start()

    @scoped
    def a_wait(*flows):
        for d, k in flows:
            a_copy(d, k, True).wait_recv()

    every = lambda k: [(d, k) for d in range(4)]

    def w_copy(d, k, got):
        sign = 1 if d == 0 else -1
        far = (k // 2 if k < 6 else 3) + (1 if got else 0)
        half = k % 2 if k < 6 else d
        here = ((z - sign * far + 8) % 8) * 2 + c
        piece = wbuf.at[here, pl.ds(half * 128, 128)]
        return remote(piece, piece, w_ssem.at[d, k], w_rsem.at[d, k], at(dz=sign))

    def b_copy(k, got):
        here = ((z + k) % 8) * 2 + ((c + 1) % 2 if got else c)
        return remote(wbuf.at[here], wbuf.at[here], b_ssem.at[k], b_rsem.at[k], at(dc=1))

    @scoped
    def w_event(k):
        for d in (0, 1):
            w_copy(d, k, True).wait_recv()
            if k < 4:
                w_copy(d, k + 2, False).start()
        if k == 4:
            w_copy(0, 6, False).start()
        if k == 5:
            w_copy(1, 6, False).start()
        if k in (1, 3, 5):
            b_copy((k + 1) // 2, False).start()
            b_copy(8 - (k + 1) // 2, False).start()
        if k == 6:
            b_copy(4, False).start()

    def row_copy(slots, ssem, rsem, k, got):
        other = (head + k) % 16
        source = (head + 16 - k) % 16
        here = source if got else head
        return remote(slots.at[here], slots.at[here], ssem.at[k], rsem.at[k], (z, c, other // 4, other % 4))

    def row_send(slots, ssem, rsem):
        def one(k, carry_):
            row_copy(slots, ssem, rsem, k, False).start()
            return carry_

        lax.fori_loop(1, 16, one, 0)

    @scoped
    def row_sum(slots, ssem, rsem):
        def one(k, carry_):
            copy = row_copy(slots, ssem, rsem, k, True)
            copy.wait_recv()
            return carry_

        lax.fori_loop(1, 16, one, 0)
        total = slots[0]
        for k in range(1, 16):
            total = total + slots[k]
        return total

    def row_done(slots, ssem, rsem):
        def one(k, carry_):
            row_copy(slots, ssem, rsem, k, False).wait_send()
            return carry_

        lax.fori_loop(1, 16, one, 0)

    def to_column(row):
        return jnp.broadcast_to(row, (128, row.shape[1])).T

    def rows128(r):
        return pl.ds(pl.multiple_of(r * 128, 128), 128)

    @scoped
    def gate_phase():
        loads[2].wait()
        loads[3].wait()

        @pl.loop(0, 8)
        def _(r):
            rows = rows128(r)
            values = so[rows, :].astype(F32)
            gate_values = gt[rows, :].astype(F32)
            sig = jax.nn.sigmoid(gate_values)
            sl = gate_values * sig
            gv = values * sl
            gated[rows, :] = gv
            silu[rows, :] = sl
            fgate[rows, :] = values * sig * (1.0 + gate_values * (1.0 - sig))
            sqs[head, :, rows] = jnp.sum(fold_lanes(gv * gv).T, axis=0, keepdims=True)

    rows_i = lax.broadcasted_iota(jnp.int32, (BLK, BLK), 0)
    cols_i = lax.broadcasted_iota(jnp.int32, (BLK, BLK), 1)

    @scoped
    def per_head():
        tri = (rows_i <= cols_i).astype(F32).astype(BF16)
        for k in range(4):
            cols = slice(k * BLK, (k + 1) * BLK)
            parts = jnp.concatenate(split3(ld_ref[:, cols]), axis=0).astype(BF16)
            summed = jnp.dot(parts, tri, preferred_element_type=F32)
            cum = summed[0:8] + summed[8:16] + summed[16:24]
            cum_s[:, cols] = cum
            total = cum[:, BLK - 1 : BLK]
            table = (
                split3(jnp.exp(cum))
                + split3(jnp.exp(total - cum))
                + split3(ts_ref[:, cols])
                + [cum, jnp.zeros((128 - CUM - 8, BLK), F32)]
            )
            qt[cols, :] = jnp.concatenate(table, axis=0).T
        lane_head = lax.broadcasted_iota(jnp.int32, (128, 512), 1) // 64
        part_row = lax.broadcasted_iota(jnp.int32, (128, 512), 0)

        for first, wide in ((ECUM, ecw), (ETAIL, etw), (TSTEP, tsw)):
            inside = (part_row >= first) & (part_row < first + 24) & ((part_row - first) % 8 == lane_head)
            chosen = inside.astype(F32).astype(BF16)

            @pl.loop(0, 4)
            def _(k, chosen=chosen, wide=wide):
                rows = pl.ds(pl.multiple_of(k * BLK, BLK), BLK)
                wide[rows, :] = jnp.dot(qt[rows, :].astype(BF16), chosen, preferred_element_type=F32)

        d0buf[0] = ecw[255:256, :] * ecw[511:512, :] * ecw[767:768, :] * ecw[1023:1024, :]

    @scoped
    def pick_group():
        group = head // 2
        for which, (load, sel) in enumerate(((loads[4], bsel), (loads[5], csel))):
            load.wait()

            @pl.loop(0, 4)
            def _(r, which=which, sel=sel):
                conv[...] = stage[which, pl.ds(pl.multiple_of(r * 2048, 2048), 2048), :].astype(F32)
                sel[pl.ds(pl.multiple_of(r * 256, 256), 256), :] = conv[pl.ds(group, 256, stride=8), :].astype(BF16)

        ct[...] = csel[...].astype(F32).T.astype(BF16)

    @scoped
    def block_weights():
        keep_upper = cols_i >= rows_i

        @pl.loop(0, 4)
        def _(k):
            rows = pl.ds(pl.multiple_of(k * BLK, BLK), BLK)
            scores = lax.dot_general(
                bsel[rows, :], csel[rows, :], (((1,), (1,)), ((), ())), preferred_element_type=F32
            )
            columns = qt[rows, :]
            for h in range(8):
                gap = cum_s[h : h + 1, rows] - columns[:, CUM + h : CUM + h + 1]
                decayed = jnp.where(keep_upper, scores * jnp.exp(jnp.minimum(gap, 0.0)), 0.0)
                wts[k, h] = decayed.astype(BF16)

    @scoped
    def normalize(mean):
        col[...] = to_column(lax.rsqrt(mean + EPS))
        nw = nw_ref[...]

        @pl.loop(0, 8)
        def _(r):
            rows = rows128(r)
            normed = gated[rows, :] * col[rows, :][:, 0:1] * nw
            normt[:, rows] = normed.T.astype(BF16)

    def pair_slots(p):
        (ex, ey), (ox, oy) = PAIRS[p]
        return slot(ex, ey), slot(ox, oy)

    def mine_and_other(p):
        first, second = pair_slots(p)
        same = (y + PAIRS[p][0][1] + 4 + c) % 2 == 0
        return jnp.where(same, first, second), jnp.where(same, second, first)

    def give_copy(p):
        return remote(gout.at[p], gin.at[p], h_ssem.at[p], h_rsem.at[p], at(dc=1))

    @scoped
    def weight_part(p):
        mine, other = mine_and_other(p)

        @pl.loop(0, 4)
        def _(r):
            rows = rows128(r)
            lhs = normt[rows, :]
            gout[p, rows, :] = jnp.dot(lhs, abuf[other], preferred_element_type=F32).astype(BF16)
            gkeep[p, rows, :] = jnp.dot(lhs, abuf[mine], preferred_element_type=F32).astype(BF16)

        give_copy(p).start()

    @scoped
    def grad_part(p):
        first, second = pair_slots(p)

        @pl.loop(0, 4)
        def _(r):
            rows = pl.ds(pl.multiple_of(r * 256, 256), 256)
            add = jnp.dot(abuf[first, rows, :], wbuf[first], preferred_element_type=F32)
            add = add + jnp.dot(abuf[second, rows, :], wbuf[second], preferred_element_type=F32)
            if p == 0:
                ng[rows, :] = add
            else:
                ng[rows, :] += add

    def among(i, values):
        found = values[0]
        for q in range(1, len(values)):
            found = jnp.where(i == q, values[q], found)
        return found

    roots = [mine_and_other(p)[0] // 2 for p in range(8)]

    def r_copy(p, i, way):
        piece = pl.ds(i * 256, 256)
        dev = ((z + jnp.where(way == 0, 1, 7)) % 8, c, x, y)
        return remote(gkeep.at[p, piece], fromz.at[way, p, piece], r_ssem.at[p, i], r_rsem.at[p, i, way], dev)

    @scoped
    def combine(p):
        give_copy(p).wait_recv()
        gkeep[p] = (gkeep[p].astype(F32) + gin[p].astype(F32)).astype(BF16)

    def rs_level(p, lev):
        rel = (z - among(p, roots) + 8) % 8
        for i in (0, 1):
            piece = pl.ds(i * 256, 256)
            way = jnp.where(rel >= 4 + i, 0, 1)
            level = jnp.where(rel >= 4 + i, rel - (4 + i), (3 + i) - rel)

            @pl.when((rel != 0) & (level == lev))
            def _():
                copy = r_copy(p, i, way)

                @pl.when(lev > 0)
                def _():
                    copy.wait_recv()
                    gkeep[p, piece, :] = (
                        gkeep[p, piece, :].astype(F32) + fromz[way, p, piece, :].astype(F32)
                    ).astype(BF16)

                copy.start()

        @pl.when((rel == 0) & (lev == 4))
        def _():
            for i in (0, 1):
                piece = pl.ds(i * 256, 256)
                r_copy(p, i, 0).wait_recv()
                r_copy(p, i, 1).wait_recv()
                total = (
                    gkeep[p, piece, :].astype(F32)
                    + fromz[0, p, piece, :].astype(F32)
                    + fromz[1, p, piece, :].astype(F32)
                )
                gw[:, i * 256 : i * 256 + 256] = total.T * (1.0 / math.sqrt(16384.0))

    @scoped
    def rs_stage(*steps):
        for p, lev in steps:
            if lev == 0:
                combine(p)
        ps, levs = [p for p, _ in steps], [lev for _, lev in steps]

        def one(i, carry_):
            rs_level(among(i, ps), among(i, levs))
            return carry_

        lax.fori_loop(0, len(steps), one, 0)

    def hop_copy(buf, ssem, rsem, way, d, got, *rest):
        source = z + (d if got else d - 1) if way == 1 else (z + 8 - (d if got else d - 1)) % 8
        here = jnp.minimum(source, 7)
        piece = buf.at[(here, *rest)]
        index = (way, d - 1)
        if rest:
            index = (way, d - 1, rest[0].start // 64)
        return remote(piece, piece, ssem.at[index], rsem.at[index], ((z + (1 if way == 0 else 7)) % 8, 1, x, y))

    def hop_valid(way, d, got):
        if way == 1:
            return (z + d <= 7) if got else ((z > 0) & (z + d - 1 <= 7))
        return (z + 8 - (d if got else d - 1)) % 8 >= 5

    WAYS = ((1, 1), (0, 1), (1, 2), (0, 2), (1, 3), (0, 3), (1, 4))
    HALVES = (pl.ds(0, 64), pl.ds(64, 64))

    def decay_copy(way, d, got):
        return hop_copy(dall, e_ssem, e_rsem, way, d, got)

    def state_copy(way, d, got, half):
        return hop_copy(sall, m_ssem, m_rsem, way, d, got, half)

    def decay_hop(d):
        @pl.when(c == 1)
        def _():
            for way in (1, 0):
                if d and (way, d) in WAYS:

                    @pl.when(hop_valid(way, d, True))
                    def _():
                        decay_copy(way, d, True).wait_recv()

                if (way, d + 1) in WAYS:

                    @pl.when(hop_valid(way, d + 1, False))
                    def _():
                        decay_copy(way, d + 1, False).start()

    @scoped
    def state_hop(d):
        for half in HALVES:
            for way in (1, 0):
                if d and (way, d) in WAYS:

                    @pl.when(hop_valid(way, d, True))
                    def _():
                        state_copy(way, d, True, half).wait_recv()

                if (way, d + 1) in WAYS:

                    @pl.when(hop_valid(way, d + 1, False))
                    def _():
                        state_copy(way, d + 1, False, half).start()

    def hops_done():
        for way, d in WAYS:

            @pl.when(hop_valid(way, d, False))
            def _():
                decay_copy(way, d, False).wait_send()
                for half in HALVES:
                    state_copy(way, d, False, half).wait_send()

    def s0_copy():
        return remote(s0buf.at[0], s0buf.at[1], s_ssem.at[0], s_rsem.at[0], (z, 1, x, y))

    def d0_copy():
        return remote(d0buf.at[0], d0buf.at[1], s_ssem.at[1], s_rsem.at[1], (z, 1, x, y))

    def core_copy():
        return remote(carry.at[0], carry.at[1], c_ssem.at[0], c_rsem.at[0], (z, 0, x, y))

    a_send(*every(0))
    for k in (0, 1):
        for d in (0, 1):
            w_copy(d, k, False).start()
    b_copy(0, False).start()
    gate_phase()
    row_send(sqs, g_ssem, g_rsem)
    a_send(*every(1))
    per_head()

    @pl.when(c == 0)
    def _():
        d0_copy().start()

    w_event(0)
    pick_group()
    w_event(1)
    a_wait(*every(0))
    a_send((0, 2), (0, 3), (0, 4), (1, 3), (3, 2), (3, 3), (3, 4), (2, 3))
    block_weights()
    w_event(2)

    @pl.when(c == 1)
    def _():
        d0_copy().wait_recv()
        dall[z] = d0buf[0] * d0buf[1]

    normalize(row_sum(sqs, g_ssem, g_rsem) * (1.0 / 8192))
    w_event(3)
    decay_hop(0)
    a_wait(*every(1))
    a_send((1, 2), (1, 4), (2, 2), (2, 4))
    weight_part(0)
    w_event(4)
    weight_part(1)
    w_event(5)
    decay_hop(1)
    a_wait((0, 2), (3, 2), (1, 3), (2, 3))
    a_send(*every(5))
    rs_stage((0, 0), (1, 0))
    w_event(6)
    decay_hop(2)
    a_wait((0, 3), (1, 2), (2, 2), (3, 3))
    a_send(*every(6))
    weight_part(2)
    with jax.named_scope("b_wait"):
        for k in range(8):
            b_copy(k, True).wait_recv()
    decay_hop(3)
    grad_part(0)
    grad_part(1)
    grad_part(2)
    decay_hop(4)
    a_wait(*every(4))
    a_send(*every(7))
    rs_stage((0, 1), (1, 1), (2, 0))
    weight_part(3)
    grad_part(3)
    weight_part(4)
    grad_part(4)
    a_wait(*every(5))
    a_send(*every(8))
    rs_stage((0, 2), (1, 2), (2, 1), (3, 0), (4, 0))
    a_wait(*every(6))
    weight_part(5)
    grad_part(5)
    a_wait(*every(7))
    grad_part(6)
    weight_part(6)
    rs_stage((0, 3), (1, 3), (2, 2), (3, 1), (4, 1), (5, 0))
    a_wait(*every(8))
    grad_part(7)

    with jax.named_scope("weighted"):

        @pl.loop(0, 8)
        def _(r):
            rows = rows128(r)
            term = nw_ref[...] * ng[rows, :] * gated[rows, :]
            wds[head, :, rows] = jnp.sum(fold_lanes(term).T, axis=0, keepdims=True)

    row_send(wds, d_ssem, d_rsem)
    weight_part(7)
    rs_stage((6, 0))

    @pl.when(c == 1)
    def _():
        weight[1] = jnp.ones((1, 512), F32)
        for k in range(2, 8):

            @pl.when(z + k <= 7)
            def _():
                weight[k] = weight[k - 1] * dall[jnp.minimum(z + k - 1, 7)]

    weighted = row_sum(wds, d_ssem, d_rsem)

    gs = gt
    with jax.named_scope("grads"):
        cube = to_column(weighted * (1.0 / 8192))
        for r in range(8):
            rows = slice(r * 128, (r + 1) * 128)
            inv = col[rows, 0:1]
            wcol = cube[rows, 0:1]
            gg = inv * nw_ref[...] * ng[rows, :] - gated[rows, :] * (inv * inv * inv * wcol)
            so[rows, :] = (gg * fgate[rows, :]).astype(BF16)
            gs[rows, :] = (gg * silu[rows, :]).astype(BF16)
    gate_out = pltpu.make_async_copy(so, gg_hbm, l_sem.at[0])
    gate_out.start()

    ends = [ecw[k * BLK + BLK - 1 : k * BLK + BLK, :] for k in range(4)]

    def summary():
        return st[0] + ends[0] * (st[1] + ends[1] * (st[2] + ends[2] * st[3]))

    with jax.named_scope("states"):

        @pl.loop(0, 4)
        def _(k):
            rows = pl.ds(pl.multiple_of(k * BLK, BLK), BLK)
            scaled = (ecw[rows, :] * gs[rows, :].astype(F32)).astype(BF16)
            st[k] = jnp.dot(ct[:, rows], scaled, preferred_element_type=F32)

    @pl.when(c == 0)
    def _():
        s0buf[0] = summary().astype(BF16)
        s0_copy().start()

    rs_stage((7, 0))

    @pl.when(c == 1)
    def _():
        own = d0buf[1] * summary()
        with jax.named_scope("s0_wait"):
            s0_copy().wait_recv()
        sall[z] = (s0buf[1].astype(F32) + own).astype(BF16)
        state_hop(0)

    @scoped
    def within_all():
        low = lax.broadcasted_iota(jnp.int32, (BLK, 128), 1) < 64

        @pl.loop(0, 4)
        def _(k):
            rows = pl.ds(pl.multiple_of(k * BLK, BLK), BLK)
            for hp in range(4):
                cols = slice(hp * 128, hp * 128 + 128)
                g = gs[rows, cols]
                zero = jnp.zeros_like(g)
                ng[rows, cols] = jnp.dot(
                    wts[k, 2 * hp], jnp.where(low, g, zero), preferred_element_type=F32
                ) + jnp.dot(wts[k, 2 * hp + 1], jnp.where(low, zero, g), preferred_element_type=F32)

    within_all()

    def take(k):
        @pl.when(z + k <= 7)
        def _():
            acc[...] += weight[k] * sall[jnp.minimum(z + k, 7)].astype(F32)

    def hop_and_take(d):
        @pl.when(c == 1)
        def _():
            state_hop(d)
            if d == 1:
                acc[...] = jnp.zeros((128, 512), F32)
            take(d)
            if d < 4:
                take(8 - d)

    hop_and_take(1)
    rs_stage((0, 4), (1, 4), (2, 3), (3, 2), (4, 2), (5, 1), (6, 1), (7, 1))
    hop_and_take(2)
    with jax.named_scope("sends_1"):
        for d in range(4):
            for k in range(9):
                a_copy(d, k, False).wait_send()
        for d in (0, 1):
            for k in range(7):
                w_copy(d, k, False).wait_send()
        for k in range(8):
            b_copy(k, False).wait_send()
        row_done(sqs, g_ssem, g_rsem)
    hop_and_take(3)
    rs_stage((2, 4), (3, 3), (4, 3), (5, 2), (6, 2), (7, 2))
    hop_and_take(4)

    @pl.when(c == 1)
    def _():
        own = st[0] + ends[0] * (st[1] + ends[1] * (st[2] + ends[2] * st[3]))
        carry[0] = (own + d0buf[0] * acc[...]).astype(BF16)
        core_copy().start()

    rs_stage((3, 4), (4, 4), (5, 3), (6, 3), (7, 3))

    @pl.when(c == 0)
    def _():
        with jax.named_scope("core_wait"):
            core_copy().wait_recv()
        acc[...] = carry[1].astype(F32)

    with jax.named_scope("final"):
        lane512 = lax.broadcasted_iota(jnp.int32, (1, 512), 1) // 64
        skw = jnp.zeros((1, 512), F32)
        for h in range(8):
            skw = jnp.where(lane512 == h, skip_ref[0, h], skw)
        gate_out.wait()
        state = acc[...]
        for k in (3, 2, 1, 0):
            rows = slice(k * BLK, (k + 1) * BLK)
            across = jnp.dot(bsel[rows, :], state.astype(BF16), preferred_element_type=F32)
            if k:
                state = st[k] + ends[k] * state
            out = tsw[rows, :] * (ng[rows, :] + etw[rows, :] * across) + skw * gs[rows, :].astype(F32)
            so[rows, :] = out.astype(BF16)
        x_out = pltpu.make_async_copy(so, gx_hbm, l_sem.at[2])
        x_out.start()

    rs_stage((5, 4), (6, 4), (7, 4))
    gw_out = pltpu.make_async_copy(gw, gw_hbm, l_sem.at[1])
    gw_out.start()

    with jax.named_scope("sends_2"):
        row_done(wds, d_ssem, d_rsem)

        def one(p, carry_):
            @pl.when((z - among(p, roots) + 8) % 8 != 0)
            def _():
                for i in (0, 1):
                    r_copy(p, i, 0).wait_send()

            give_copy(p).wait_send()
            return carry_

        lax.fori_loop(0, 8, one, 0)

        @pl.when(c == 0)
        def _():
            d0_copy().wait_send()
            s0_copy().wait_send()

        @pl.when(c == 1)
        def _():
            core_copy().wait_send()
            hops_done()

        gw_out.wait()
        x_out.wait()


def on_device(a, w, so, gt, nw, ts, ld, bin_, cin, skip):
    any_ = pl.BlockSpec(memory_space=pl.ANY)
    vmem = pl.BlockSpec(memory_space=pltpu.VMEM)
    smem = pl.BlockSpec(memory_space=pltpu.SMEM)
    V, D = pltpu.VMEM, pltpu.SemaphoreType.DMA
    return pl.pallas_call(
        kernel,
        out_shape=(
            jax.ShapeDtypeStruct((1024, 512), BF16),
            jax.ShapeDtypeStruct((1024, 512), BF16),
            jax.ShapeDtypeStruct((256, 512), F32),
        ),
        in_specs=[any_, any_, any_, any_, vmem, vmem, vmem, any_, any_, smem],
        out_specs=(any_, any_, any_),
        scratch_shapes=[
            V((16, 1024, 256), BF16), V((16, 256, 512), BF16), V((1024, 512), BF16), V((1024, 512), BF16),
            V((1024, 512), F32), V((1024, 512), F32), V((1024, 512), F32), V((1024, 512), F32),
            V((1024, 512), F32), V((1024, 512), F32), V((1024, 512), F32), V((4, 8, 256, 256), BF16),
            V((8, 512, 256), BF16), V((8, 512, 256), BF16), V((8, 512, 256), BF16), V((2, 8, 512, 256), BF16),
            V((512, 1024), BF16), V((2, 8192, 128), BF16), V((2048, 128), F32), V((1024, 128), BF16),
            V((1024, 128), BF16), V((128, 1024), BF16), V((1024, 128), F32), V((8, 1024), F32), V((1024, 128), F32),
            V((16, 1, 1024), F32), V((16, 1, 1024), F32), V((4, 128, 512), F32), V((128, 512), F32),
            V((2, 128, 512), BF16), V((2, 1, 512), F32), V((8, 128, 512), BF16), V((8, 1, 512), F32),
            V((8, 1, 512), F32), V((2, 128, 512), BF16), V((256, 512), F32),
            D((4, 9)), D((4, 9)), D((2, 7)), D((2, 7)), D((8,)), D((8,)), D((8, 2)), D((8, 2, 2)), D((16,)), D((16,)),
            D((8,)), D((8,)), D((16,)), D((16,)), D((2,)), D((2,)), D((1,)), D((1,)), D((2, 4, 2)), D((2, 4, 2)),
            D((2, 4)), D((2, 4)), D((6,)),
        ],
        compiler_params=pltpu.CompilerParams(
            collective_id=0, has_side_effects=True, vmem_limit_bytes=67043328
        ),
        name="mixer_backward",
    )(
        a, w, so, gt, nw.reshape(1, 512), ts, ld, bin_.reshape(8192, 128), cin.reshape(8192, 128), skip.reshape(1, 8)
    )


def solution(mesh):
    finer = Mesh(mesh.devices.reshape(8, 2, 4, 4), ("z", "c", "x", "y"))
    seq, heads = ("z", "c"), ("x", "y")
    return jax.shard_map(
        on_device,
        mesh=finer,
        in_specs=(
            P(seq, heads), P(seq, heads), P(seq, heads), P(seq, heads), P(heads), P(heads, seq), P(heads, seq),
            P(seq, None, None), P(seq, None, None), P(heads),
        ),
        out_specs=(P(seq, heads), P(seq, heads), P(seq, heads)),
        check_vma=False,
    )
```

```python
import functools
import math

import jax
import jax.numpy as jnp
from jax import lax
from jax.experimental import pallas as pl
from jax.experimental.pallas import tpu as pltpu
from jax.sharding import Mesh
from jax.sharding import PartitionSpec as P

EPS = 1e-05
F32, BF16 = jnp.float32, jnp.bfloat16
MESH = pl.DeviceIdType.MESH
BLK = 256
A, B = (0, 512), (512, 512)
A0, A1, B0, B1 = (0, 256), (256, 256), (512, 256), (768, 256)
STEP = ((1, 0), (-1, 0), (0, 1), (0, -1))
ITEMS = (
    ((0, 0, A), (0, 0, B), (-1, 0, A), (0, 1, B), (0, -1, B), (0, 2, B0), (-1, 1, B0), (-1, -1, B0), (-1, 2, B0), (0, 2, B1)),
    ((0, 0, A), (0, 0, B), (1, 0, B), (0, 1, B), (0, -1, B), (0, 2, B1), (1, 1, B1), (1, -1, B1), (1, 2, B1), (0, 2, B0)),
    ((0, 0, B), (0, 0, A), (0, -1, A), (1, 0, A), (-1, 0, A), (2, 0, A), (1, -1, A0), (-1, -1, A0), (2, -1, A0)),
    ((0, 0, B), (0, 0, A), (0, 1, B), (1, 0, A), (-1, 0, A), (2, 0, A), (1, 1, A1), (-1, 1, A1), (2, 1, A1)),
)
BLOCKS = (
    (0, 0), (0, 1), (1, 0), (0, -1), (-1, 0),
    (2, 0), (0, 2), (1, 1),
    (-1, 1), (1, -1), (-1, -1),
    (2, 1), (2, -1),
    (1, 2), (-1, 2),
    (2, 2),
)
SPLIT = 8
G0, G1, G2, G3, G4 = range(0, 5), range(5, 8), range(8, 11), range(11, 13), range(13, 16)
G0A, G0B = (0, 2, 4), (1, 3)
CUTS = [1] * 13 + [4] * 3
ECUM, ETAIL, TSTEP, CUM = 0, 24, 48, 72


def split3(q):
    first = q.astype(BF16).astype(F32)
    second = (q - first).astype(BF16).astype(F32)
    third = (q - first - second).astype(BF16).astype(F32)
    return [first, second, third]


def scoped(fn):
    @functools.wraps(fn)
    def wrapped(*args):
        with jax.named_scope(fn.__name__):
            return fn(*args)

    return wrapped


def fold_lanes(v):
    return (v[:, 0:128] + v[:, 128:256]) + (v[:, 256:384] + v[:, 384:512])


def kernel(
    a_hbm, w_hbm, so_hbm, gt_hbm, nw_ref, ts_ref, ld_ref, bin_hbm, cin_hbm, skip_ref,
    gx_hbm, gg_hbm, gw_hbm,
    abuf, wbuf, so, gt, gated, silu, fgate, ng, ecw, etw, tsw, wts, gkeep, gin, fromz, rootb,
    normt, conv, bsel, csel, ct, qt, cum_s, col, sqs, wds, st, acc, s0buf, d0buf, sall, dall, weight, carry, gw,
    a_ssem, a_rsem, w_ssem, w_rsem, b_ssem, b_rsem, r_ssem, r_rsem, g_ssem, g_rsem, h_ssem, h_rsem,
    d_ssem, d_rsem, s_ssem, s_rsem, c_ssem, c_rsem, m_ssem, m_rsem, e_ssem, e_rsem, o_ssem, o_rsem, l_sem,
):
    z, c, x, y = (lax.axis_index(n) for n in ("z", "c", "x", "y"))
    head = x * 4 + y

    def at(dz=0, dc=0, dx=0, dy=0):
        return ((z + dz + 8) & 7, (c + dc) & 1, (x + dx + 4) & 3, (y + dy + 4) & 3)

    def slot(dx, dy):
        return ((x + dx + 4) & 3) * 4 + ((y + dy + 4) & 3)

    def remote(src, dst, ssem, rsem, dev):
        return pltpu.make_async_remote_copy(
            src_ref=src, dst_ref=dst, send_sem=ssem, recv_sem=rsem, device_id=dev, device_id_type=MESH
        )

    loads = [
        pltpu.make_async_copy(a_hbm, abuf.at[head], l_sem.at[0]),
        pltpu.make_async_copy(w_hbm, wbuf.at[z * 2 + c], l_sem.at[1]),
        pltpu.make_async_copy(so_hbm, so, l_sem.at[2]),
        pltpu.make_async_copy(gt_hbm, gt, l_sem.at[3]),
        pltpu.make_async_copy(bin_hbm, wts.at[:, 0:128], l_sem.at[4]),
        pltpu.make_async_copy(cin_hbm, wts.at[:, 128:256], l_sem.at[5]),
    ]
    for load in loads:
        load.start()
    barrier = pltpu.get_barrier_semaphore()

    def greet(k, carry_):
        other = (head + k) & 15
        pl.semaphore_signal(barrier, inc=1, device_id=(z, c, other >> 2, other & 3), device_id_type=MESH)
        return carry_

    lax.fori_loop(1, 16, greet, 0)
    for dev in (at(dz=1), at(dz=-1), at(dc=1)):
        pl.semaphore_signal(barrier, inc=1, device_id=dev, device_id_type=MESH)
    with jax.named_scope("entry"):
        loads[0].wait()
        loads[1].wait()
        pl.semaphore_wait(barrier, 18)

    def a_copy(d, k, got):
        dx, dy, (row, n) = ITEMS[d][k]
        sx, sy = STEP[d]
        here = slot(dx - sx, dy - sy) if got else slot(dx, dy)
        piece = abuf.at[here, pl.ds(row, n)]
        return remote(piece, piece, a_ssem.at[d, k], a_rsem.at[d, k], at(dx=sx, dy=sy))

    def a_send(*flows):
        for d, k in flows:
            a_copy(d, k, False).start()

    @scoped
    def a_wait(*flows):
        for d, k in flows:
            a_copy(d, k, True).wait_recv()

    every = lambda k: [(d, k) for d in range(4)]

    def w_copy(d, k, got):
        sign = 1 if d == 0 else -1
        far = (k // 2 if k < 6 else 3) + (1 if got else 0)
        half = k % 2 if k < 6 else d
        here = ((z - sign * far + 8) & 7) * 2 + c
        piece = wbuf.at[here, pl.ds(half * 128, 128)]
        return remote(piece, piece, w_ssem.at[d, k], w_rsem.at[d, k], at(dz=sign))

    def b_copy(k, got):
        here = ((z + k) & 7) * 2 + ((1 - c) if got else c)
        return remote(wbuf.at[here], wbuf.at[here], b_ssem.at[k], b_rsem.at[k], at(dc=1))

    @scoped
    def w_event(k):
        for d in (0, 1):
            w_copy(d, k, True).wait_recv()
            if k < 4:
                w_copy(d, k + 2, False).start()
        if k == 4:
            w_copy(0, 6, False).start()
        if k == 5:
            w_copy(1, 6, False).start()
        if k in (1, 3, 5):
            b_copy((k + 1) // 2, False).start()
            b_copy(8 - (k + 1) // 2, False).start()
        if k == 6:
            b_copy(4, False).start()

    def row_copy(slots, ssem, rsem, k, got):
        other = (head + k) & 15
        source = (head + 16 - k) & 15
        here = source if got else head
        return remote(slots.at[here], slots.at[here], ssem.at[k], rsem.at[k], (z, c, other >> 2, other & 3))

    def row_send(slots, ssem, rsem):
        def one(k, carry_):
            row_copy(slots, ssem, rsem, k, False).start()
            return carry_

        lax.fori_loop(1, 16, one, 0)

    @scoped
    def row_sum(slots, ssem, rsem):
        def one(k, carry_):
            copy = row_copy(slots, ssem, rsem, k, True)
            copy.wait_recv()
            return carry_

        lax.fori_loop(1, 16, one, 0)
        total = slots[0]
        for k in range(1, 16):
            total = total + slots[k]
        return total

    def row_done(slots, ssem, rsem):
        def one(k, carry_):
            row_copy(slots, ssem, rsem, k, False).wait_send()
            return carry_

        lax.fori_loop(1, 16, one, 0)

    def to_column(row):
        return jnp.broadcast_to(row, (128, row.shape[1])).T

    def rows128(r):
        return pl.ds(pl.multiple_of(r * 128, 128), 128)

    @scoped
    def gate_phase():
        loads[2].wait()
        loads[3].wait()

        @pl.loop(0, 8)
        def _(r):
            rows = rows128(r)
            values = so[rows, :].astype(F32)
            gate_values = gt[rows, :].astype(F32)
            sig = jax.nn.sigmoid(gate_values)
            sl = gate_values * sig
            gv = values * sl
            gated[rows, :] = gv
            silu[rows, :] = sl
            fgate[rows, :] = values * sig * (1.0 + gate_values * (1.0 - sig))
            sqs[head, :, rows] = jnp.sum(fold_lanes(gv * gv).T, axis=0, keepdims=True)

    rows_i = lax.broadcasted_iota(jnp.int32, (BLK, BLK), 0)
    cols_i = lax.broadcasted_iota(jnp.int32, (BLK, BLK), 1)

    @scoped
    def per_head():
        tri = (rows_i <= cols_i).astype(F32).astype(BF16)
        for k in range(4):
            cols = slice(k * BLK, (k + 1) * BLK)
            parts = jnp.concatenate(split3(ld_ref[:, cols]), axis=0).astype(BF16)
            summed = jnp.dot(parts, tri, preferred_element_type=F32)
            cum = summed[0:8] + summed[8:16] + summed[16:24]
            cum_s[:, cols] = cum
            total = cum[:, BLK - 1 : BLK]
            table = (
                split3(jnp.exp(cum))
                + split3(jnp.exp(total - cum))
                + split3(ts_ref[:, cols])
                + [cum, jnp.zeros((128 - CUM - 8, BLK), F32)]
            )
            qt[cols, :] = jnp.concatenate(table, axis=0).T
        lane_head = lax.broadcasted_iota(jnp.int32, (128, 512), 1) // 64
        part_row = lax.broadcasted_iota(jnp.int32, (128, 512), 0)

        for first, wide in ((ECUM, ecw), (ETAIL, etw), (TSTEP, tsw)):
            inside = (part_row >= first) & (part_row < first + 24) & ((part_row - first) % 8 == lane_head)
            chosen = inside.astype(F32).astype(BF16)

            @pl.loop(0, 4)
            def _(k, chosen=chosen, wide=wide):
                rows = pl.ds(pl.multiple_of(k * BLK, BLK), BLK)
                wide[rows, :] = jnp.dot(qt[rows, :].astype(BF16), chosen, preferred_element_type=F32)

        d0buf[0] = ecw[255:256, :] * ecw[511:512, :] * ecw[767:768, :] * ecw[1023:1024, :]

    @scoped
    def pick_group():
        group = head // 2
        for which, (load, sel) in enumerate(((loads[4], bsel), (loads[5], csel))):
            load.wait()

            @pl.loop(0, 4)
            def _(r, which=which, sel=sel):
                conv[...] = wts[pl.ds(pl.multiple_of(r * 2048, 2048), 2048), which * 128 : which * 128 + 128].astype(F32)
                sel[pl.ds(pl.multiple_of(r * 256, 256), 256), :] = conv[pl.ds(group, 256, stride=8), :].astype(BF16)

        ct[...] = csel[...].astype(F32).T.astype(BF16)

    @scoped
    def block_weights():
        keep_upper = cols_i >= rows_i

        @pl.loop(0, 4)
        def _(k):
            rows = pl.ds(pl.multiple_of(k * BLK, BLK), BLK)
            scores = lax.dot_general(
                bsel[rows, :], csel[rows, :], (((1,), (1,)), ((), ())), preferred_element_type=F32
            )
            columns = qt[rows, :]
            for h in range(8):
                gap = cum_s[h : h + 1, rows] - columns[:, CUM + h : CUM + h + 1]
                decayed = jnp.where(keep_upper, scores * jnp.exp(jnp.minimum(gap, 0.0)), 0.0)
                wts[pl.ds(pl.multiple_of(k * 2048 + h * 256, 256), 256), :] = decayed.astype(BF16)

    @scoped
    def normalize(mean):
        col[...] = to_column(lax.rsqrt(mean + EPS))
        nw = nw_ref[...]

        @pl.loop(0, 8)
        def _(r):
            rows = rows128(r)
            normed = gated[rows, :] * col[rows, :][:, 0:1] * nw
            normt[:, rows] = normed.T.astype(BF16)

    owners = [slot(*block) for block in BLOCKS]

    def give_copy(q):
        return remote(gkeep.at[q], gin.at[q], h_ssem.at[q], h_rsem.at[q], at(dc=1))

    def kept(q):
        return (owners[q] & 1) == c if q < SPLIT else c == 0

    def given(q):
        return (owners[q] & 1) != c if q < SPLIT else c == 1

    @scoped
    def weight_part(group):
        @pl.loop(0, 4)
        def _(r):
            rows = rows128(r)
            lhs = normt[rows, :]
            for q in group:
                gkeep[q, rows, :] = jnp.dot(lhs, abuf[owners[q]], preferred_element_type=F32).astype(BF16)

        for q in group:

            @pl.when(given(q))
            def _():
                give_copy(q).start()

    @scoped
    def grad_part(group):
        @pl.loop(0, 4)
        def _(r):
            rows = pl.ds(pl.multiple_of(r * 256, 256), 256)
            add = None if 0 in group else ng[rows, :]
            for q in group:
                more = jnp.dot(abuf[owners[q], rows, :], wbuf[owners[q]], preferred_element_type=F32)
                add = more if add is None else add + more
            ng[rows, :] = add

    def r_copy(q, i, n, way, last=None):
        size = 256 // CUTS[q]
        piece = pl.ds(pl.multiple_of(i * 256 + n * size, size), size)
        dev = ((z + jnp.where(way == 0, 1, 7)) & 7, c, x, y)
        dst = fromz.at[q, piece] if last is None else rootb.at[last, piece]
        return remote(gkeep.at[q, piece], dst, r_ssem.at[q, i, n], r_rsem.at[q, i, way, n], dev)

    def cuts(q, fn):
        if CUTS[q] == 1:
            fn(0)
        else:
            pl.loop(0, CUTS[q])(fn)

    def add_rows(q, row, n, term):
        step = min(n, 64)

        @pl.loop(0, n // step)
        def _(r):
            rows = pl.ds(pl.multiple_of(row + r * step, step), step)
            gkeep[q, rows, :] = (gkeep[q, rows, :].astype(F32) + term[q, rows, :].astype(F32)).astype(BF16)

    def rs_level(q, lev):
        owner = owners[q]
        rel = (z - (owner >> 1) + 8) & 7
        which = owner & 1
        if lev == 0:
            give_copy(q).wait_recv()
            add_rows(q, 0, 512, gin)
        if lev == 4:

            @pl.when(rel == 0)
            def _():
                for i in (0, 1):

                    @functools.partial(cuts, q)
                    def _(n):
                        r_copy(q, i, n, 0).wait_recv()
                        r_copy(q, i, n, 1, which).wait_recv()

                @pl.loop(0, 4)
                def _(r):
                    rows = rows128(r)
                    total = (
                        gkeep[q, rows, :].astype(F32)
                        + fromz[q, rows, :].astype(F32)
                        + rootb[which, rows, :].astype(F32)
                    )
                    gw[which, :, rows] = total.T * (1.0 / math.sqrt(16384.0))

            return
        for i in (0, 1):
            high, low = 4 + i + lev, 3 + i - lev
            here = rel == high if high <= 7 else None
            if low >= 1:
                here = (rel == low) if here is None else here | (rel == low)
            if here is None:
                continue

            @pl.when(here)
            def _():
                way = jnp.where(rel >= 4 + i, 0, 1)

                @functools.partial(cuts, q)
                def _(n):
                    if lev:
                        r_copy(q, i, n, way).wait_recv()
                        size = 256 // CUTS[q]
                        add_rows(q, i * 256 + n * size, size, fromz)

                    @pl.when(rel == 1)
                    def _():
                        r_copy(q, i, n, way, which).start()

                    @pl.when(rel != 1)
                    def _():
                        r_copy(q, i, n, way).start()

    @scoped
    def rs_stage(*steps):
        for group, lev in steps:
            for q in group:

                @pl.when(kept(q))
                def _():
                    rs_level(q, lev)

    handed = owners[SPLIT] == 2 * z + 1
    for q in range(SPLIT + 1, 16):
        handed = handed | (owners[q] == 2 * z + 1)

    def out_copy():
        return remote(gw.at[1], gw.at[1], o_ssem.at[0], o_rsem.at[0], (z, 1, x, y))

    def hop_copy(buf, ssem, rsem, way, d, got, *rest):
        source = z + (d if got else d - 1) if way == 1 else ((z + 8 - (d if got else d - 1)) & 7)
        here = jnp.minimum(source, 7)
        piece = buf.at[(here, *rest)]
        index = (way, d - 1)
        if rest:
            index = (way, d - 1, rest[0].start // 16)
        return remote(piece, piece, ssem.at[index], rsem.at[index], ((z + (1 if way == 0 else 7)) & 7, 1, x, y))

    def hop_valid(way, d, got):
        if way == 1:
            return (z + d <= 7) if got else ((z > 0) & (z + d - 1 <= 7))
        return ((z + 8 - (d if got else d - 1)) & 7) >= 5

    WAYS = ((1, 1), (0, 1), (1, 2), (0, 2), (1, 3), (0, 3), (1, 4))
    HALVES = [pl.ds(16 * i, 16) for i in range(8)]

    def decay_copy(way, d, got):
        return hop_copy(dall, e_ssem, e_rsem, way, d, got)

    def state_copy(way, d, got, half):
        return hop_copy(sall, m_ssem, m_rsem, way, d, got, half)

    def decay_hop(d):
        @pl.when(c == 1)
        def _():
            for way in (1, 0):
                if d and (way, d) in WAYS:

                    @pl.when(hop_valid(way, d, True))
                    def _():
                        decay_copy(way, d, True).wait_recv()

                if (way, d + 1) in WAYS:

                    @pl.when(hop_valid(way, d + 1, False))
                    def _():
                        decay_copy(way, d + 1, False).start()

    @scoped
    def state_hop(d):
        for half in HALVES:
            for way in (1, 0):
                if d and (way, d) in WAYS:

                    @pl.when(hop_valid(way, d, True))
                    def _():
                        state_copy(way, d, True, half).wait_recv()

                if (way, d + 1) in WAYS:

                    @pl.when(hop_valid(way, d + 1, False))
                    def _():
                        state_copy(way, d + 1, False, half).start()

    def hops_done():
        for way, d in WAYS:

            @pl.when(hop_valid(way, d, False))
            def _():
                decay_copy(way, d, False).wait_send()
                for half in HALVES:
                    state_copy(way, d, False, half).wait_send()

    def s0_copy():
        return remote(s0buf.at[0], s0buf.at[1], s_ssem.at[0], s_rsem.at[0], (z, 1, x, y))

    def d0_copy():
        return remote(d0buf.at[0], d0buf.at[1], s_ssem.at[1], s_rsem.at[1], (z, 1, x, y))

    def core_copy():
        return remote(carry.at[0], carry.at[1], c_ssem.at[0], c_rsem.at[0], (z, 0, x, y))

    a_send(*every(0))
    for k in (0, 1):
        for d in (0, 1):
            w_copy(d, k, False).start()
    b_copy(0, False).start()
    gate_phase()
    row_send(sqs, g_ssem, g_rsem)
    a_send(*every(1))
    per_head()

    @pl.when(c == 0)
    def _():
        d0_copy().start()

    w_event(0)
    pick_group()
    w_event(1)
    a_wait(*every(0))
    a_send((0, 2), (0, 3), (0, 4), (1, 3), (3, 2), (3, 3), (3, 4), (2, 3))
    block_weights()
    w_event(2)

    @pl.when(c == 1)
    def _():
        d0_copy().wait_recv()
        dall[z] = d0buf[0] * d0buf[1]

    normalize(row_sum(sqs, g_ssem, g_rsem) * (1.0 / 8192))
    w_event(3)
    decay_hop(0)
    a_wait(*every(1))
    a_send((1, 2), (1, 4), (2, 2), (2, 4))
    weight_part(G0)
    w_event(4)
    w_event(5)
    decay_hop(1)
    a_wait((0, 2), (3, 2), (1, 3), (2, 3))
    a_send((2, 5), (3, 5), (1, 6))
    rs_stage((G0A, 0))
    w_event(6)
    decay_hop(2)
    a_wait((0, 3), (1, 2), (2, 2), (3, 3))
    a_send((0, 6), (2, 6), (3, 6))
    rs_stage((G0B, 0))
    weight_part(G1)
    with jax.named_scope("b_wait"):
        for k in range(8):
            b_copy(k, True).wait_recv()
    grad_part(range(0, 4))
    rs_stage((G0A, 1), (G1, 0))
    a_wait(*every(4))
    a_send((0, 7), (1, 7), (2, 7), (3, 7), (0, 5), (1, 5), (0, 9), (1, 9))
    grad_part(range(4, 8))
    decay_hop(3)
    rs_stage((G0B, 1))
    weight_part(G2)
    rs_stage((G0A, 2))
    grad_part(G2)
    a_wait((0, 6), (1, 6), (0, 7), (1, 7), (2, 5), (3, 5))
    a_send((2, 8), (3, 8))
    rs_stage((G1, 1), (G2, 0))
    weight_part(G3)
    decay_hop(4)
    rs_stage((G0B, 2))
    a_wait((0, 5), (1, 5), (2, 6), (3, 6))
    a_send((0, 8), (1, 8))
    grad_part(G3)
    rs_stage((G0A, 3), (G3, 0))
    a_wait((0, 9), (1, 9), (2, 7), (3, 7))
    grad_part(range(13, 15))
    rs_stage((G1, 2), (G2, 1))
    a_wait(*every(8))

    with jax.named_scope("weighted"):
        last = owners[15]

        @pl.loop(0, 4)
        def _(r):
            rows = pl.ds(pl.multiple_of(r * 256, 256), 256)
            done = ng[rows, :] + jnp.dot(abuf[last, rows, :], wbuf[last], preferred_element_type=F32)
            ng[rows, :] = done
            term = nw_ref[...] * done * gated[rows, :]
            wds[head, :, rows] = jnp.sum(fold_lanes(term).T, axis=0, keepdims=True)

    row_send(wds, d_ssem, d_rsem)
    weight_part(G4)
    rs_stage((G4, 0), (G0B, 3), (G3, 1), (G1, 3), (G2, 2))

    @pl.when(c == 1)
    def _():
        weight[1] = jnp.ones((1, 512), F32)
        for k in range(2, 8):

            @pl.when(z + k <= 7)
            def _():
                weight[k] = weight[k - 1] * dall[jnp.minimum(z + k - 1, 7)]

    weighted = row_sum(wds, d_ssem, d_rsem)

    gs = gt
    with jax.named_scope("grads"):
        cube = to_column(weighted * (1.0 / 8192))
        for r in range(8):
            rows = slice(r * 128, (r + 1) * 128)
            inv = col[rows, 0:1]
            wcol = cube[rows, 0:1]
            gg = inv * nw_ref[...] * ng[rows, :] - gated[rows, :] * (inv * inv * inv * wcol)
            so[rows, :] = (gg * fgate[rows, :]).astype(BF16)
            gs[rows, :] = (gg * silu[rows, :]).astype(BF16)
    gate_out = pltpu.make_async_copy(so, gg_hbm, l_sem.at[0])
    gate_out.start()

    ends = [ecw[k * BLK + BLK - 1 : k * BLK + BLK, :] for k in range(4)]

    def summary():
        return st[0] + ends[0] * (st[1] + ends[1] * (st[2] + ends[2] * st[3]))

    with jax.named_scope("states"):

        @pl.loop(0, 4)
        def _(k):
            rows = pl.ds(pl.multiple_of(k * BLK, BLK), BLK)
            scaled = (ecw[rows, :] * gs[rows, :].astype(F32)).astype(BF16)
            st[k] = jnp.dot(ct[:, rows], scaled, preferred_element_type=F32)

    @pl.when(c == 0)
    def _():
        s0buf[0] = summary().astype(BF16)
        s0_copy().start()

    @scoped
    def within_all():
        low = lax.broadcasted_iota(jnp.int32, (BLK, 128), 1) < 64

        @pl.loop(0, 4)
        def _(k):
            rows = pl.ds(pl.multiple_of(k * BLK, BLK), BLK)
            for hp in range(4):
                cols = slice(hp * 128, hp * 128 + 128)
                g = gs[rows, cols]
                zero = jnp.zeros_like(g)
                even, odd = (wts[pl.ds(pl.multiple_of(k * 2048 + h * 256, 256), 256), :] for h in (2 * hp, 2 * hp + 1))
                ng[rows, cols] = jnp.dot(even, jnp.where(low, g, zero), preferred_element_type=F32) + jnp.dot(
                    odd, jnp.where(low, zero, g), preferred_element_type=F32
                )

    rs_stage((G4, 1), (G3, 2))
    within_all()
    rs_stage((G2, 3))

    @pl.when(c == 1)
    def _():
        own = d0buf[1] * summary()
        with jax.named_scope("s0_wait"):
            s0_copy().wait_recv()
        sall[z] = (s0buf[1].astype(F32) + own).astype(BF16)
        state_hop(0)

    def take(k):
        @pl.when(z + k <= 7)
        def _():
            acc[...] += weight[k] * sall[jnp.minimum(z + k, 7)].astype(F32)

    def hop_and_take(d):
        @pl.when(c == 1)
        def _():
            state_hop(d)
            if d == 1:
                acc[...] = jnp.zeros((128, 512), F32)
            take(d)
            if d < 4:
                take(8 - d)

    with jax.named_scope("sends_1"):
        for d in range(4):
            for k in range(len(ITEMS[d])):
                a_copy(d, k, False).wait_send()
        for d in (0, 1):
            for k in range(7):
                w_copy(d, k, False).wait_send()
        for k in range(8):
            b_copy(k, False).wait_send()
        row_done(sqs, g_ssem, g_rsem)
        row_done(wds, d_ssem, d_rsem)
    for d in (1, 2, 3, 4):
        hop_and_take(d)

    @pl.when(c == 1)
    def _():
        own = st[0] + ends[0] * (st[1] + ends[1] * (st[2] + ends[2] * st[3]))
        carry[0] = (own + d0buf[0] * acc[...]).astype(BF16)
        core_copy().start()

    rs_stage((G4, 2), (G3, 3), (G0A, 4), (G0B, 4))
    rs_stage((G4, 3), (G1, 4), (G2, 4), (G3, 4), (G4, 4))

    @pl.when((c == 0) & handed)
    def _():
        out_copy().start()

    @pl.when(c == 0)
    def _():
        with jax.named_scope("core_wait"):
            core_copy().wait_recv()
        acc[...] = carry[1].astype(F32)

    with jax.named_scope("final"):
        lane512 = lax.broadcasted_iota(jnp.int32, (1, 512), 1) // 64
        skw = jnp.zeros((1, 512), F32)
        for h in range(8):
            skw = jnp.where(lane512 == h, skip_ref[0, h], skw)
        gate_out.wait()
        state = acc[...]
        x_outs = []
        for k in (3, 2, 1, 0):
            rows = slice(k * BLK, (k + 1) * BLK)
            across = jnp.dot(bsel[rows, :], state.astype(BF16), preferred_element_type=F32)
            if k:
                state = st[k] + ends[k] * state
            out = tsw[rows, :] * (ng[rows, :] + etw[rows, :] * across) + skw * gs[rows, :].astype(F32)
            so[rows, :] = out.astype(BF16)
            x_out = pltpu.make_async_copy(so.at[rows], gx_hbm.at[rows], l_sem.at[2 + k])
            x_out.start()
            x_outs.append(x_out)

    @pl.when((c == 1) & handed)
    def _():
        with jax.named_scope("out_wait"):
            out_copy().wait_recv()

    gw_out = pltpu.make_async_copy(gw.at[c], gw_hbm, l_sem.at[1])
    gw_out.start()

    with jax.named_scope("sends_2"):

        @pl.when(c == 0)
        def _():
            d0_copy().wait_send()
            s0_copy().wait_send()

            @pl.when(handed)
            def _():
                out_copy().wait_send()

        @pl.when(c == 1)
        def _():
            core_copy().wait_send()
            hops_done()

        for q in range(16):

            @pl.when(given(q))
            def _():
                give_copy(q).wait_send()

            @pl.when(kept(q) & (((z - (owners[q] >> 1) + 8) & 7) != 0))
            def _():
                for i in (0, 1):

                    @functools.partial(cuts, q)
                    def _(n):
                        r_copy(q, i, n, 0).wait_send()

        gw_out.wait()
        for x_out in x_outs:
            x_out.wait()


def move(*refs):
    ins, outs, bufs, (in_sem, out_sem) = refs[:3], refs[3:6], refs[6:9], refs[9:]
    steps = []
    for k in range(3):
        n = ins[k].shape[0] // 4
        for r in range(4):
            rows = pl.ds(r * n, n)
            steps.append(
                (
                    pltpu.make_async_copy(ins[k].at[rows], bufs[k].at[rows], in_sem.at[k, r]),
                    pltpu.make_async_copy(bufs[k].at[rows], outs[k].at[rows], out_sem.at[k, r]),
                )
            )
    for first, _ in steps:
        first.start()
    for first, second in steps:
        first.wait()
        second.start()
    for _, second in steps:
        second.wait()


def on_device(a, w, so, gt, nw, ts, ld, bin_, cin, skip):
    any_ = pl.BlockSpec(memory_space=pl.ANY)
    vmem = pl.BlockSpec(memory_space=pltpu.VMEM)
    smem = pl.BlockSpec(memory_space=pltpu.SMEM)
    V, D = pltpu.VMEM, pltpu.SemaphoreType.DMA
    results = pl.pallas_call(
        kernel,
        out_shape=(
            jax.ShapeDtypeStruct((1024, 512), BF16),
            jax.ShapeDtypeStruct((1024, 512), BF16),
            jax.ShapeDtypeStruct((256, 512), F32),
        ),
        in_specs=[any_, any_, any_, any_, vmem, vmem, vmem, any_, any_, smem],
        out_specs=(any_, any_, any_),
        scratch_shapes=[
            V((16, 1024, 256), BF16), V((16, 256, 512), BF16), V((1024, 512), BF16), V((1024, 512), BF16),
            V((1024, 512), F32), V((1024, 512), F32), V((1024, 512), F32), V((1024, 512), F32),
            V((1024, 512), F32), V((1024, 512), F32), V((1024, 512), F32), V((8192, 256), BF16),
            V((16, 512, 256), BF16), V((16, 512, 256), BF16), V((16, 512, 256), BF16), V((2, 512, 256), BF16),
            V((512, 1024), BF16), V((2048, 128), F32), V((1024, 128), BF16),
            V((1024, 128), BF16), V((128, 1024), BF16), V((1024, 128), F32), V((8, 1024), F32), V((1024, 128), F32),
            V((16, 1, 1024), F32), V((16, 1, 1024), F32), V((4, 128, 512), F32), V((128, 512), F32),
            V((2, 128, 512), BF16), V((2, 1, 512), F32), V((8, 128, 512), BF16), V((8, 1, 512), F32),
            V((8, 1, 512), F32), V((2, 128, 512), BF16), V((2, 256, 512), F32),
            D((4, 10)), D((4, 10)), D((2, 7)), D((2, 7)), D((8,)), D((8,)), D((16, 2, 4)), D((16, 2, 2, 4)), D((16,)), D((16,)),
            D((16,)), D((16,)), D((16,)), D((16,)), D((2,)), D((2,)), D((1,)), D((1,)), D((2, 4, 8)), D((2, 4, 8)),
            D((2, 4)), D((2, 4)), D((1,)), D((1,)), D((6,)),
        ],
        compiler_params=pltpu.CompilerParams(
            collective_id=0, has_side_effects=True, vmem_limit_bytes=59768832
        ),
        name="mixer_backward",
    )(
        a, w, so, gt, nw.reshape(1, 512), ts, ld, bin_.reshape(8192, 128), cin.reshape(8192, 128), skip.reshape(1, 8)
    )
    V, D = pltpu.VMEM, pltpu.SemaphoreType.DMA
    return pl.pallas_call(
        move,
        out_shape=[jax.ShapeDtypeStruct(r.shape, r.dtype) for r in results],
        in_specs=[any_] * 3,
        out_specs=[any_] * 3,
        scratch_shapes=[V(r.shape, r.dtype) for r in results] + [D((3, 4)), D((3, 4))],
        compiler_params=pltpu.CompilerParams(vmem_limit_bytes=62914560),
        name="move",
    )(*results)


def solution(mesh):
    finer = Mesh(mesh.devices.reshape(8, 2, 4, 4), ("z", "c", "x", "y"))
    seq, heads = ("z", "c"), ("x", "y")
    return jax.shard_map(
        on_device,
        mesh=finer,
        in_specs=(
            P(seq, heads), P(seq, heads), P(seq, heads), P(seq, heads), P(heads), P(heads, seq), P(heads, seq),
            P(seq, None, None), P(seq, None, None), P(heads),
        ),
        out_specs=(P(seq, heads), P(seq, heads), P(seq, heads)),
        check_vma=False,
    )
```

```python
import functools
import math

import jax
import jax.numpy as jnp
from jax import lax
from jax.experimental import pallas as pl
from jax.experimental.pallas import tpu as pltpu
from jax.sharding import Mesh
from jax.sharding import PartitionSpec as P

EPS = 1e-05
F32, BF16 = jnp.float32, jnp.bfloat16
MESH = pl.DeviceIdType.MESH
BLK = 256
A, B = (0, 512), (512, 512)
A0, A1, B0, B1 = (0, 256), (256, 256), (512, 256), (768, 256)
STEP = ((1, 0), (-1, 0), (0, 1), (0, -1))
ITEMS = (
    ((0, 0, A), (0, 0, B), (-1, 0, A), (0, 1, B), (0, -1, B), (0, 2, B0), (-1, 1, B0), (-1, -1, B0), (-1, 2, B0), (0, 2, B1)),
    ((0, 0, A), (0, 0, B), (1, 0, B), (0, 1, B), (0, -1, B), (0, 2, B1), (1, 1, B1), (1, -1, B1), (1, 2, B1), (0, 2, B0)),
    ((0, 0, B), (0, 0, A), (0, -1, A), (1, 0, A), (-1, 0, A), (2, 0, A), (1, -1, A0), (-1, -1, A0), (2, -1, A0)),
    ((0, 0, B), (0, 0, A), (0, 1, B), (1, 0, A), (-1, 0, A), (2, 0, A), (1, 1, A1), (-1, 1, A1), (2, 1, A1)),
)
EVENTS = (
    (((0, 0), (1, 0), (2, 0), (3, 0)), 2),
    (((0, 1), (1, 1), (2, 1), (3, 1)), 2),
    (((0, 2), (3, 2), (1, 3), (2, 3)), 2),
    (((0, 3), (1, 2), (2, 2), (3, 3)), 2),
    (((0, 4), (1, 4), (2, 4), (3, 4)), 2),
    (((0, 6), (1, 6), (0, 7), (1, 7), (2, 5), (3, 5)), 2),
    (((0, 5), (1, 5), (2, 6), (3, 6)), 1),
    (((0, 9), (1, 9), (2, 7), (3, 7)), 1),
    (((0, 8), (1, 8), (2, 8), (3, 8)), 1),
)
EVENT_OF = {flow: e for e, (flows, _) in enumerate(EVENTS) for flow in flows}
BLOCKS = (
    (0, 0), (0, 1), (1, 0), (0, -1), (-1, 0),
    (2, 0), (0, 2), (1, 1),
    (-1, 1), (1, -1), (-1, -1),
    (2, 1), (2, -1),
    (1, 2), (-1, 2),
    (2, 2),
)
SPLIT = 8
G0, G1, G2, G3, G4 = range(0, 5), range(5, 8), range(8, 11), range(11, 13), range(13, 16)
G0A, G0B = (0, 2, 4), (1, 3)
CUTS = [1] * 13 + [4] * 3
ECUM, ETAIL, TSTEP, CUM = 0, 24, 48, 72


def split3(q):
    first = q.astype(BF16).astype(F32)
    second = (q - first).astype(BF16).astype(F32)
    third = (q - first - second).astype(BF16).astype(F32)
    return [first, second, third]


def scoped(fn):
    @functools.wraps(fn)
    def wrapped(*args):
        with jax.named_scope(fn.__name__):
            return fn(*args)

    return wrapped


def fold_lanes(v):
    return (v[:, 0:128] + v[:, 128:256]) + (v[:, 256:384] + v[:, 384:512])


def kernel(
    a_hbm, w_hbm, so_hbm, gt_hbm, nw_ref, ts_ref, ld_ref, bin_hbm, cin_hbm, skip_ref,
    gx_hbm, gg_hbm, gw_hbm,
    abuf, wbuf, so, gt, gated, silu, fgate, ng, ecw, etw, tsw, wts, gkeep, gin, fromz, rootb,
    normt, conv, bsel, csel, ct, qt, cum_s, col, sqs, wds, st, acc, s0buf, d0buf, schip, legs, mout, vout, decays, carry, gw,
    a_ssem, a_rsem, w_ssem, w_rsem, b_rsem, r_ssem, r_rsem, g_ssem, g_rsem, h_rsem,
    d_ssem, d_rsem, s_ssem, s_rsem, c_ssem, c_rsem, m_ssem, m_rsem, e_ssem, e_rsem, o_ssem, o_rsem, l_sem,
):
    z, c, x, y = (lax.axis_index(n) for n in ("z", "c", "x", "y"))
    head = x * 4 + y

    def at(dz=0, dc=0, dx=0, dy=0):
        return ((z + dz + 8) & 7, (c + dc) & 1, (x + dx + 4) & 3, (y + dy + 4) & 3)

    def slot(dx, dy):
        return ((x + dx + 4) & 3) * 4 + ((y + dy + 4) & 3)

    def remote(src, dst, ssem, rsem, dev):
        return pltpu.make_async_remote_copy(
            src_ref=src, dst_ref=dst, send_sem=ssem, recv_sem=rsem, device_id=dev, device_id_type=MESH
        )

    loads = [
        pltpu.make_async_copy(a_hbm, abuf.at[head], l_sem.at[0]),
        pltpu.make_async_copy(w_hbm, wbuf.at[z * 2 + c], l_sem.at[1]),
        pltpu.make_async_copy(so_hbm, so, l_sem.at[2]),
        pltpu.make_async_copy(gt_hbm, gt, l_sem.at[3]),
        pltpu.make_async_copy(bin_hbm, wts.at[:, 0:128], l_sem.at[4]),
        pltpu.make_async_copy(cin_hbm, wts.at[:, 128:256], l_sem.at[5]),
    ]
    for load in loads:
        load.start()
    barrier = pltpu.get_barrier_semaphore()

    def greet(k, carry_):
        other = (head + k) & 15
        pl.semaphore_signal(barrier, inc=1, device_id=(z, c, other >> 2, other & 3), device_id_type=MESH)
        return carry_

    lax.fori_loop(1, 16, greet, 0)
    for dev in (at(dz=1), at(dz=-1), at(dc=1)):
        pl.semaphore_signal(barrier, inc=1, device_id=dev, device_id_type=MESH)
    with jax.named_scope("entry"):
        loads[0].wait()
        loads[1].wait()
        pl.semaphore_wait(barrier, 18)

    def a_send(*flows):
        for d, k in flows:
            dx, dy, (row, n) = ITEMS[d][k]
            sx, sy = STEP[d]
            piece = abuf.at[slot(dx, dy), pl.ds(row, n)]
            remote(piece, piece, a_ssem.at[0], a_rsem.at[EVENT_OF[d, k]], at(dx=sx, dy=sy)).start()

    def whole(buf, n, sem):
        part = buf.at[pl.ds(0, n)]
        pltpu.make_async_copy(part, part, sem).wait()

    @scoped
    def a_wait(event):
        whole(abuf, EVENTS[event][1], a_rsem.at[event])

    every = lambda k: [(d, k) for d in range(4)]

    def w_copy(d, k):
        sign = 1 if d == 0 else -1
        far = k // 2 if k < 6 else 3
        half = k % 2 if k < 6 else d
        here = ((z - sign * far + 8) & 7) * 2 + c
        piece = wbuf.at[here, pl.ds(half * 128, 128)]
        return remote(piece, piece, w_ssem.at[0], w_rsem.at[k], at(dz=sign))

    def b_copy(k):
        here = ((z + k) & 7) * 2 + c
        return remote(wbuf.at[here], wbuf.at[here], w_ssem.at[0], b_rsem.at[0], at(dc=1))

    @scoped
    def w_event(k):
        whole(wbuf, 1, w_rsem.at[k])
        if k < 4:
            for d in (0, 1):
                w_copy(d, k + 2).start()
        if k == 4:
            w_copy(0, 6).start()
        if k == 5:
            w_copy(1, 6).start()
        if k in (1, 3, 5):
            b_copy((k + 1) // 2).start()
            b_copy(8 - (k + 1) // 2).start()
        if k == 6:
            b_copy(4).start()

    def row_send(slots, ssem, rsem):
        def one(k, carry_):
            other = (head + k) & 15
            here = slots.at[head]
            remote(here, here, ssem.at[0], rsem.at[0], (z, c, other >> 2, other & 3)).start()
            return carry_

        lax.fori_loop(1, 16, one, 0)

    @scoped
    def row_sum(slots, rsem):
        whole(slots, 15, rsem.at[0])
        total = slots[0]
        for k in range(1, 16):
            total = total + slots[k]
        return total

    def to_column(row):
        return jnp.broadcast_to(row, (128, row.shape[1])).T

    def rows128(r):
        return pl.ds(pl.multiple_of(r * 128, 128), 128)

    @scoped
    def gate_phase():
        loads[2].wait()
        loads[3].wait()

        @pl.loop(0, 8)
        def _(r):
            rows = rows128(r)
            values = so[rows, :].astype(F32)
            gate_values = gt[rows, :].astype(F32)
            sig = jax.nn.sigmoid(gate_values)
            sl = gate_values * sig
            gv = values * sl
            gated[rows, :] = gv
            silu[rows, :] = sl
            fgate[rows, :] = values * sig * (1.0 + gate_values * (1.0 - sig))
            sqs[head, :, rows] = jnp.sum(fold_lanes(gv * gv).T, axis=0, keepdims=True)

    rows_i = lax.broadcasted_iota(jnp.int32, (BLK, BLK), 0)
    cols_i = lax.broadcasted_iota(jnp.int32, (BLK, BLK), 1)

    @scoped
    def per_head():
        tri = (rows_i <= cols_i).astype(F32).astype(BF16)
        for k in range(4):
            cols = slice(k * BLK, (k + 1) * BLK)
            parts = jnp.concatenate(split3(ld_ref[:, cols]), axis=0).astype(BF16)
            summed = jnp.dot(parts, tri, preferred_element_type=F32)
            cum = summed[0:8] + summed[8:16] + summed[16:24]
            cum_s[:, cols] = cum
            total = cum[:, BLK - 1 : BLK]
            table = (
                split3(jnp.exp(cum))
                + split3(jnp.exp(total - cum))
                + split3(ts_ref[:, cols])
                + [cum, jnp.zeros((128 - CUM - 8, BLK), F32)]
            )
            qt[cols, :] = jnp.concatenate(table, axis=0).T
        lane_head = lax.broadcasted_iota(jnp.int32, (128, 512), 1) // 64
        part_row = lax.broadcasted_iota(jnp.int32, (128, 512), 0)

        for first, wide in ((ECUM, ecw), (ETAIL, etw), (TSTEP, tsw)):
            inside = (part_row >= first) & (part_row < first + 24) & ((part_row - first) % 8 == lane_head)
            chosen = inside.astype(F32).astype(BF16)

            @pl.loop(0, 4)
            def _(k, chosen=chosen, wide=wide):
                rows = pl.ds(pl.multiple_of(k * BLK, BLK), BLK)
                wide[rows, :] = jnp.dot(qt[rows, :].astype(BF16), chosen, preferred_element_type=F32)

        d0buf[0] = ecw[255:256, :] * ecw[511:512, :] * ecw[767:768, :] * ecw[1023:1024, :]

    @scoped
    def pick_group():
        group = head // 2
        for which, (load, sel) in enumerate(((loads[4], bsel), (loads[5], csel))):
            load.wait()

            @pl.loop(0, 4)
            def _(r, which=which, sel=sel):
                conv[...] = wts[pl.ds(pl.multiple_of(r * 2048, 2048), 2048), which * 128 : which * 128 + 128].astype(F32)
                sel[pl.ds(pl.multiple_of(r * 256, 256), 256), :] = conv[pl.ds(group, 256, stride=8), :].astype(BF16)

        ct[...] = csel[...].astype(F32).T.astype(BF16)

    @scoped
    def block_weights():
        keep_upper = cols_i >= rows_i

        @pl.loop(0, 4)
        def _(k):
            rows = pl.ds(pl.multiple_of(k * BLK, BLK), BLK)
            scores = lax.dot_general(
                bsel[rows, :], csel[rows, :], (((1,), (1,)), ((), ())), preferred_element_type=F32
            )
            columns = qt[rows, :]
            for h in range(8):
                gap = cum_s[h : h + 1, rows] - columns[:, CUM + h : CUM + h + 1]
                decayed = jnp.where(keep_upper, scores * jnp.exp(jnp.minimum(gap, 0.0)), 0.0)
                wts[pl.ds(pl.multiple_of(k * 2048 + h * 256, 256), 256), :] = decayed.astype(BF16)

    @scoped
    def normalize(mean):
        col[...] = to_column(lax.rsqrt(mean + EPS))
        nw = nw_ref[...]

        @pl.loop(0, 8)
        def _(r):
            rows = rows128(r)
            normed = gated[rows, :] * col[rows, :][:, 0:1] * nw
            normt[:, rows] = normed.T.astype(BF16)

    owners = [slot(*block) for block in BLOCKS]

    def give_copy(q):
        return remote(gkeep.at[q], gin.at[q], r_ssem.at[q], h_rsem.at[q], at(dc=1))

    def kept(q):
        return (owners[q] & 1) == c if q < SPLIT else c == 0

    def given(q):
        return (owners[q] & 1) != c if q < SPLIT else c == 1

    @scoped
    def weight_part(group):
        @pl.loop(0, 4)
        def _(r):
            rows = rows128(r)
            lhs = normt[rows, :]
            for q in group:
                gkeep[q, rows, :] = jnp.dot(lhs, abuf[owners[q]], preferred_element_type=F32).astype(BF16)

        for q in group:

            @pl.when(given(q))
            def _():
                give_copy(q).start()

    @scoped
    def grad_part(group):
        @pl.loop(0, 4)
        def _(r):
            rows = pl.ds(pl.multiple_of(r * 256, 256), 256)
            add = None if 0 in group else ng[rows, :]
            for q in group:
                more = jnp.dot(abuf[owners[q], rows, :], wbuf[owners[q]], preferred_element_type=F32)
                add = more if add is None else add + more
            ng[rows, :] = add

    def r_copy(q, i, n, way, last=None):
        size = 256 // CUTS[q]
        piece = pl.ds(pl.multiple_of(i * 256 + n * size, size), size)
        dev = ((z + jnp.where(way == 0, 1, 7)) & 7, c, x, y)
        src = gkeep.at[q, piece]
        if last is not None:
            return remote(src, rootb.at[last, piece], r_ssem.at[q], o_rsem.at[last], dev)
        flow = 2 * q + i if q < 13 else 26 + (q - 13) * 8 + i * 4 + n
        return remote(src, fromz.at[q, piece], r_ssem.at[q], r_rsem.at[flow], dev)

    def cuts(q, fn):
        if CUTS[q] == 1:
            fn(0)
        else:
            pl.loop(0, CUTS[q])(fn)

    def add_rows(q, row, n, term):
        step = min(n, 64)

        @pl.loop(0, n // step)
        def _(r):
            rows = pl.ds(pl.multiple_of(row + r * step, step), step)
            gkeep[q, rows, :] = (gkeep[q, rows, :].astype(F32) + term[q, rows, :].astype(F32)).astype(BF16)

    def from_core(q):
        give_copy(q).wait_recv()
        add_rows(q, 0, 512, gin)

    def rs_root(q):
        which = owners[q] & 1

        @pl.when(z == (owners[q] >> 1))
        def _():
            for i in (0, 1):

                @functools.partial(cuts, q)
                def _(n):
                    r_copy(q, i, n, 0).wait_recv()

            there = rootb.at[which]
            pltpu.make_async_copy(there, there, o_rsem.at[which]).wait()

            @pl.loop(0, 4)
            def _(r):
                rows = rows128(r)
                total = (
                    gkeep[q, rows, :].astype(F32)
                    + fromz[q, rows, :].astype(F32)
                    + rootb[which, rows, :].astype(F32)
                )
                gw[which, :, rows] = total.T * (1.0 / math.sqrt(16384.0))

    def rs_piece(q, i, n, lev):
        rel = (z - (owners[q] >> 1) + 8) & 7
        high, low = 4 + i + lev, 3 + i - lev
        here = rel == high if high <= 7 else None
        if low >= 1:
            here = (rel == low) if here is None else here | (rel == low)
        if here is None:
            return

        @pl.when(here)
        def _():
            way = jnp.where(rel >= 4 + i, 0, 1)
            if lev:
                r_copy(q, i, n, way).wait_recv()
                size = 256 // CUTS[q]
                add_rows(q, i * 256 + n * size, size, fromz)

            @pl.when(rel == 1)
            def _():
                r_copy(q, i, n, way, owners[q] & 1).start()

            @pl.when(rel != 1)
            def _():
                r_copy(q, i, n, way).start()

    @scoped
    def rs_stage(*steps):
        for group, lev in steps:
            if group == G4:

                @pl.when(c == 0)
                def _():
                    if lev == 4:
                        for q in group:
                            rs_root(q)
                        return
                    if lev == 0:
                        for q in group:
                            from_core(q)

                    @pl.loop(0, 4)
                    def _(n):
                        for i in (0, 1):
                            for q in group:
                                rs_piece(q, i, n, lev)

                continue
            for q in group:

                @pl.when(kept(q))
                def _():
                    if lev == 4:
                        rs_root(q)
                        return
                    if lev == 0:
                        from_core(q)
                    for i in (0, 1):
                        rs_piece(q, i, 0, lev)

    handed = owners[SPLIT] == 2 * z + 1
    for q in range(SPLIT + 1, 16):
        handed = handed | (owners[q] == 2 * z + 1)

    def out_copy():
        return remote(gw.at[1], gw_hbm, o_ssem.at[0], o_rsem.at[2], (z, 1, x, y))

    QUARTERS = [pl.ds(32 * i, 32) for i in range(4)]
    X, V, R = range(3)

    def leg(src, kind, q, dz):
        return remote(
            src.at[QUARTERS[q]], legs.at[kind, QUARTERS[q]], m_ssem.at[kind], m_rsem.at[kind, q], at(dz=dz)
        )

    def leg_wait(kind, q):
        part = legs.at[kind, QUARTERS[q]]
        pltpu.make_async_copy(part, part, m_rsem.at[kind, q]).wait()

    def decay_hop(d):
        @pl.when((c == 1) & ((z == 4 + d) | (z == 3 - d)))
        def _():
            onward = remote(
                decays.at[2], decays.at[1], e_ssem.at[0], e_rsem.at[0], ((z + jnp.where(z >= 4, 1, 7)) & 7, 1, x, y)
            )
            if d:
                onward.wait_recv()
            else:
                decays[1] = jnp.ones((1, 512), F32)
            if d < 3:
                decays[2] = decays[1] * decays[0]
                onward.start()

    def down_task(q):
        piece = QUARTERS[q]
        leg_wait(X, q)
        mout[piece, :] = (schip[piece, :] + decays[0] * legs[X, piece, :].astype(F32)).astype(BF16)

        @pl.when(z == 4)
        def _():
            leg(mout, R, q, -1).start()

        @pl.when(z != 4)
        def _():
            leg(mout, X, q, -1).start()

    def up_task(q):
        piece = QUARTERS[q]
        leg_wait(V, q)
        vout[piece, :] = (legs[V, piece, :].astype(F32) + decays[1] * schip[piece, :]).astype(BF16)

        @pl.when(z == 7)
        def _():
            leg(vout, R, q, 1).start()

        @pl.when(z != 7)
        def _():
            leg(vout, V, q, 1).start()

    def quarters(when, fn):
        @pl.when(when)
        def _():
            for q in range(4):
                fn(q)

    @scoped
    def exchange():
        for q in range(4):
            piece = QUARTERS[q]

            @pl.when((z == 7) | (z == 3))
            def _():
                mout[piece, :] = schip[piece, :].astype(BF16)
                leg(mout, X, q, -1).start()

            @pl.when(z == 4)
            def _():
                vout[piece, :] = schip[piece, :].astype(BF16)
                leg(vout, V, q, 1).start()

    @scoped
    def exchange_rest():
        quarters((z == 6) | (z == 2), down_task)
        quarters(z == 5, up_task)
        quarters((z == 5) | (z == 1), down_task)
        quarters(z == 6, up_task)
        quarters(z == 4, down_task)
        quarters(z == 7, up_task)
        quarters(z == 0, lambda q: leg_wait(X, q))

        def pass_on(dz):
            def fn(q):
                leg_wait(R, q)
                leg(legs.at[R], R, q, dz).start()

            return fn

        quarters(z == 3, pass_on(-1))
        quarters(z == 0, pass_on(1))
        quarters((z == 2) | (z == 1), lambda q: leg_wait(R, q))

        @pl.when(z == 7)
        def _():
            acc[...] = jnp.zeros((128, 512), F32)

        @pl.when((z >= 4) & (z < 7))
        def _():
            acc[...] = legs[X].astype(F32)

        @pl.when(z == 3)
        def _():
            acc[...] = legs[R].astype(F32)

        @pl.when(z < 3)
        def _():
            acc[...] = legs[X].astype(F32) + decays[1] * legs[R].astype(F32)

    def exchange_sent():
        def sent(kind):
            pltpu.make_async_copy(legs.at[kind], legs.at[kind], m_ssem.at[kind]).wait()

        @pl.when((z != 0) & (z != 4))
        def _():
            sent(X)

        @pl.when((z >= 4) & (z < 7))
        def _():
            sent(V)

        @pl.when((z == 4) | (z == 7) | (z == 3) | (z == 0))
        def _():
            sent(R)

        @pl.when((z != 7) & (z != 0))
        def _():
            pltpu.make_async_copy(decays.at[2], decays.at[2], e_ssem.at[0]).wait()

    def s0_copy():
        return remote(s0buf.at[0], s0buf.at[1], s_ssem.at[0], s_rsem.at[0], (z, 1, x, y))

    def d0_copy():
        return remote(d0buf.at[0], d0buf.at[1], s_ssem.at[1], s_rsem.at[1], (z, 1, x, y))

    def core_copy():
        return remote(carry.at[0], carry.at[1], c_ssem.at[0], c_rsem.at[0], (z, 0, x, y))

    a_send(*every(0))
    for k in (0, 1):
        for d in (0, 1):
            w_copy(d, k).start()
    b_copy(0).start()
    gate_phase()
    row_send(sqs, g_ssem, g_rsem)
    a_send(*every(1))
    per_head()

    @pl.when(c == 0)
    def _():
        d0_copy().start()

    w_event(0)
    pick_group()
    w_event(1)
    a_wait(0)
    a_send((0, 2), (0, 3), (0, 4), (1, 3), (3, 2), (3, 3), (3, 4), (2, 3))
    block_weights()
    w_event(2)

    @pl.when(c == 1)
    def _():
        d0_copy().wait_recv()
        decays[0] = d0buf[0] * d0buf[1]

    normalize(row_sum(sqs, g_rsem) * (1.0 / 8192))
    w_event(3)
    decay_hop(0)
    a_wait(1)
    a_send((1, 2), (1, 4), (2, 2), (2, 4))
    weight_part(G0A)
    weight_part(G0B)
    w_event(4)
    w_event(5)
    rs_stage((G0A, 0))
    decay_hop(1)
    a_wait(2)
    a_send((2, 5), (3, 5), (1, 6))
    w_event(6)
    rs_stage((G0B, 0))
    decay_hop(2)
    a_wait(3)
    a_send((0, 6), (2, 6), (3, 6))
    rs_stage((G0A, 1))
    weight_part(G1)
    with jax.named_scope("b_wait"):
        whole(wbuf, 8, b_rsem.at[0])
    grad_part(range(0, 4))
    rs_stage((G0B, 1), (G1, 0))
    decay_hop(3)
    a_wait(4)
    a_send((0, 7), (1, 7), (2, 7), (3, 7), (0, 5), (1, 5), (0, 9), (1, 9))
    grad_part(range(4, 8))
    rs_stage((G0A, 2))
    weight_part(G2)
    grad_part(G2)
    rs_stage((G0B, 2), (G1, 1))
    a_wait(5)
    a_send((2, 8), (3, 8))
    rs_stage((G2, 0))
    weight_part(G3)
    rs_stage((G0A, 3))
    a_wait(6)
    a_send((0, 8), (1, 8))
    grad_part(G3)
    rs_stage((G3, 0))
    a_wait(7)
    grad_part(range(13, 15))
    a_wait(8)

    with jax.named_scope("weighted"):
        last = owners[15]

        @pl.loop(0, 4)
        def _(r):
            rows = pl.ds(pl.multiple_of(r * 256, 256), 256)
            done = ng[rows, :] + jnp.dot(abuf[last, rows, :], wbuf[last], preferred_element_type=F32)
            ng[rows, :] = done
            term = nw_ref[...] * done * gated[rows, :]
            wds[head, :, rows] = jnp.sum(fold_lanes(term).T, axis=0, keepdims=True)

    row_send(wds, d_ssem, d_rsem)
    rs_stage((G0B, 3), (G1, 2), (G2, 1))
    weight_part(G4)
    rs_stage((G4, 0), (G3, 1))

    weighted = row_sum(wds, d_rsem)

    gs = gt
    with jax.named_scope("grads"):
        cube = to_column(weighted * (1.0 / 8192))
        for r in range(8):
            rows = slice(r * 128, (r + 1) * 128)
            inv = col[rows, 0:1]
            wcol = cube[rows, 0:1]
            gg = inv * nw_ref[...] * ng[rows, :] - gated[rows, :] * (inv * inv * inv * wcol)
            so[rows, :] = (gg * fgate[rows, :]).astype(BF16)
            gs[rows, :] = (gg * silu[rows, :]).astype(BF16)
    gate_out = pltpu.make_async_copy(so, gg_hbm, l_sem.at[0])
    gate_out.start()

    ends = [ecw[k * BLK + BLK - 1 : k * BLK + BLK, :] for k in range(4)]

    def summary():
        return st[0] + ends[0] * (st[1] + ends[1] * (st[2] + ends[2] * st[3]))

    with jax.named_scope("states"):

        @pl.loop(0, 4)
        def _(k):
            rows = pl.ds(pl.multiple_of(k * BLK, BLK), BLK)
            scaled = (ecw[rows, :] * gs[rows, :].astype(F32)).astype(BF16)
            st[k] = jnp.dot(ct[:, rows], scaled, preferred_element_type=F32)

    @pl.when(c == 0)
    def _():
        s0buf[0] = summary().astype(BF16)
        s0_copy().start()

    @scoped
    def within_all():
        low = lax.broadcasted_iota(jnp.int32, (BLK, 128), 1) < 64

        @pl.loop(0, 4)
        def _(k):
            rows = pl.ds(pl.multiple_of(k * BLK, BLK), BLK)
            for hp in range(4):
                cols = slice(hp * 128, hp * 128 + 128)
                g = gs[rows, cols]
                zero = jnp.zeros_like(g)
                even, odd = (wts[pl.ds(pl.multiple_of(k * 2048 + h * 256, 256), 256), :] for h in (2 * hp, 2 * hp + 1))
                ng[rows, cols] = jnp.dot(even, jnp.where(low, g, zero), preferred_element_type=F32) + jnp.dot(
                    odd, jnp.where(low, zero, g), preferred_element_type=F32
                )

    rs_stage((G4, 1))
    within_all()
    rs_stage((G1, 3), (G3, 2), (G2, 2), (G0A, 4))

    @pl.when(c == 1)
    def _():
        own = d0buf[1] * summary()
        with jax.named_scope("s0_wait"):
            s0_copy().wait_recv()
        schip[...] = s0buf[1].astype(F32) + own
        exchange()

    with jax.named_scope("sends_1"):
        whole(abuf, 15, a_ssem.at[0])
        whole(wbuf, 15, w_ssem.at[0])
        whole(sqs, 15, g_ssem.at[0])
        whole(wds, 15, d_ssem.at[0])
    pl.when(c == 1)(exchange_rest)

    @pl.when(c == 1)
    def _():
        own = st[0] + ends[0] * (st[1] + ends[1] * (st[2] + ends[2] * st[3]))
        carry[0] = (own + d0buf[0] * acc[...]).astype(BF16)
        core_copy().start()

    rs_stage((G4, 2), (G2, 3), (G3, 3), (G0B, 4))
    rs_stage((G4, 3), (G1, 4), (G2, 4), (G3, 4), (G4, 4))

    @pl.when((c == 0) & handed)
    def _():
        out_copy().start()

    @pl.when(c == 0)
    def _():
        with jax.named_scope("core_wait"):
            core_copy().wait_recv()
        acc[...] = carry[1].astype(F32)

    with jax.named_scope("final"):
        lane512 = lax.broadcasted_iota(jnp.int32, (1, 512), 1) // 64
        skw = jnp.zeros((1, 512), F32)
        for h in range(8):
            skw = jnp.where(lane512 == h, skip_ref[0, h], skw)
        gate_out.wait()
        state = acc[...]
        x_outs = []
        for k in (3, 2, 1, 0):
            rows = slice(k * BLK, (k + 1) * BLK)
            across = jnp.dot(bsel[rows, :], state.astype(BF16), preferred_element_type=F32)
            if k:
                state = st[k] + ends[k] * state
            out = tsw[rows, :] * (ng[rows, :] + etw[rows, :] * across) + skw * gs[rows, :].astype(F32)
            so[rows, :] = out.astype(BF16)
            x_out = pltpu.make_async_copy(so.at[rows], gx_hbm.at[rows], l_sem.at[2 + k])
            x_out.start()
            x_outs.append(x_out)

    gw_out = pltpu.make_async_copy(gw.at[c], gw_hbm, l_sem.at[1])
    own_rows = (c == 0) | jnp.logical_not(handed)

    @pl.when(own_rows)
    def _():
        gw_out.start()


    with jax.named_scope("sends_2"):

        @pl.when(c == 0)
        def _():
            d0_copy().wait_send()
            s0_copy().wait_send()

            @pl.when(handed)
            def _():
                out_copy().wait_send()

        @pl.when(c == 1)
        def _():
            core_copy().wait_send()
            exchange_sent()

        for q in range(16):

            @pl.when(given(q) | (((z - (owners[q] >> 1) + 8) & 7) != 0))
            def _():
                give_copy(q).wait_send()

        @pl.when((c == 1) & handed)
        def _():
            with jax.named_scope("out_wait"):
                out_copy().wait_recv()

        @pl.when(own_rows)
        def _():
            gw_out.wait()

        for x_out in x_outs:
            x_out.wait()


def move(*refs):
    ins, outs, bufs, (in_sem, out_sem) = refs[:3], refs[3:6], refs[6:9], refs[9:]
    steps = []
    for k in range(3):
        n = ins[k].shape[0] // 4
        for r in range(4):
            rows = pl.ds(r * n, n)
            steps.append(
                (
                    pltpu.make_async_copy(ins[k].at[rows], bufs[k].at[rows], in_sem.at[k, r]),
                    pltpu.make_async_copy(bufs[k].at[rows], outs[k].at[rows], out_sem.at[k]),
                )
            )
    for first, _ in steps:
        first.start()
    for first, second in steps:
        first.wait()
        second.start()
    for k in range(3):
        pltpu.make_async_copy(bufs[k], outs[k], out_sem.at[k]).wait()


def on_device(a, w, so, gt, nw, ts, ld, bin_, cin, skip):
    any_ = pl.BlockSpec(memory_space=pl.ANY)
    vmem = pl.BlockSpec(memory_space=pltpu.VMEM)
    smem = pl.BlockSpec(memory_space=pltpu.SMEM)
    V, D = pltpu.VMEM, pltpu.SemaphoreType.DMA
    results = pl.pallas_call(
        kernel,
        out_shape=(
            jax.ShapeDtypeStruct((1024, 512), BF16),
            jax.ShapeDtypeStruct((1024, 512), BF16),
            jax.ShapeDtypeStruct((256, 512), F32),
        ),
        in_specs=[any_, any_, any_, any_, vmem, vmem, vmem, any_, any_, smem],
        out_specs=(any_, any_, any_),
        scratch_shapes=[
            V((16, 1024, 256), BF16), V((16, 256, 512), BF16), V((1024, 512), BF16), V((1024, 512), BF16),
            V((1024, 512), F32), V((1024, 512), F32), V((1024, 512), F32), V((1024, 512), F32),
            V((1024, 512), F32), V((1024, 512), F32), V((1024, 512), F32), V((8192, 256), BF16),
            V((16, 512, 256), BF16), V((16, 512, 256), BF16), V((16, 512, 256), BF16), V((2, 512, 256), BF16),
            V((512, 1024), BF16), V((2048, 128), F32), V((1024, 128), BF16),
            V((1024, 128), BF16), V((128, 1024), BF16), V((1024, 128), F32), V((8, 1024), F32), V((1024, 128), F32),
            V((16, 1, 1024), F32), V((16, 1, 1024), F32), V((4, 128, 512), F32), V((128, 512), F32),
            V((2, 128, 512), BF16), V((2, 1, 512), F32), V((128, 512), F32),
            V((3, 128, 512), BF16), V((128, 512), BF16), V((128, 512), BF16), V((3, 1, 512), F32), V((2, 128, 512), BF16), V((2, 256, 512), F32),
            D((1,)), D((9,)), D((1,)), D((7,)), D((1,)), D((16,)), D((50,)), D((1,)), D((1,)), D((16,)),
            D((1,)), D((1,)), D((2,)), D((2,)), D((1,)), D((1,)), D((3,)), D((3, 4)), D((1,)), D((1,)), D((1,)), D((3,)),
            D((6,)),
        ],
        compiler_params=pltpu.CompilerParams(
            collective_id=0, has_side_effects=True, vmem_limit_bytes=59768832
        ),
        name="mixer_backward",
    )(
        a, w, so, gt, nw.reshape(1, 512), ts, ld, bin_.reshape(8192, 128), cin.reshape(8192, 128), skip.reshape(1, 8)
    )
    V, D = pltpu.VMEM, pltpu.SemaphoreType.DMA
    return pl.pallas_call(
        move,
        out_shape=[jax.ShapeDtypeStruct(r.shape, r.dtype) for r in results],
        in_specs=[any_] * 3,
        out_specs=[any_] * 3,
        scratch_shapes=[V(r.shape, r.dtype) for r in results] + [D((3, 4)), D((3,))],
        compiler_params=pltpu.CompilerParams(vmem_limit_bytes=62914560),
        name="move",
    )(*results)


def solution(mesh):
    finer = Mesh(mesh.devices.reshape(8, 2, 4, 4), ("z", "c", "x", "y"))
    seq, heads = ("z", "c"), ("x", "y")
    return jax.shard_map(
        on_device,
        mesh=finer,
        in_specs=(
            P(seq, heads), P(seq, heads), P(seq, heads), P(seq, heads), P(heads), P(heads, seq), P(heads, seq),
            P(seq, None, None), P(seq, None, None), P(heads),
        ),
        out_specs=(P(seq, heads), P(seq, heads), P(seq, heads)),
        check_vma=False,
    )
```
